128 devices in a mesh: dp: 1, ep: 128 (over z, y, x, core).
Axes of the slice: x: 4, y: 4, z: 4, core: 2. Of those that a mesh axis runs over, the one named last changes fastest.
Arguments:
- tokens: bfloat16 [65536, 1024], P(('dp', 'ep'))
- slot_ids: int32 [65536, 4, 32], P(('dp', 'ep'))
- request_rows: int32 [128, 128, 64], P(('dp', 'ep'))
- gate_vals: float32 [65536, 4, 32], P(('dp', 'ep'))
- grad_out: bfloat16 [65536, 1024], P(('dp', 'ep'))
- table_up: bfloat16 [16384, 1024], P('ep')
- table_down: bfloat16 [16384, 1024], P('ep')
Outputs:
- output 1: bfloat16 [65536, 1024], P(('dp', 'ep'))
- output 2: bfloat16 [65536, 1024], P(('dp', 'ep'))
- output 3: bfloat16 [16384, 1024], P(('dp', 'ep'))
- output 4: bfloat16 [16384, 1024], P(('dp', 'ep'))
All inputs are finite; a program needn't handle non-finite values.
Results may differ from the reference program's by a relative error of at most 0.00849675.
Values are sent between devices in bfloat16 or wider.
A program may use at most 1 GiB of HBM per device.

```python
import math
import jax
import jax.numpy as jnp
from jax import lax

TOKENS_DEV = 512
DISTINCT = 64
GROUP_SIZE = 128
EXPERTS = 16384
MODEL_DIM = 1024
NUM_HEADS = 4
TOP_K = 32


def draw_routing(route_key):
    rows_owner = EXPERTS // GROUP_SIZE
    sel_dev = TOKENS_DEV * NUM_HEADS * TOP_K
    slots_dev = GROUP_SIZE * DISTINCT
    hot_slots = max(1, DISTINCT // 8)
    sub_keys = jax.random.split(route_key, 9)
    owner_perm = jax.vmap(lambda one_key: jax.random.permutation(one_key, rows_owner))(jax.random.split(sub_keys[0], GROUP_SIZE))
    hot_first = jax.random.randint(sub_keys[1], (), 0, GROUP_SIZE)
    hot_second = (hot_first + 1 + jax.random.randint(sub_keys[2], (), 0, GROUP_SIZE - 1)) % GROUP_SIZE
    owner_iota = jnp.arange(GROUP_SIZE)
    hot_owner = (owner_iota == hot_first) | (owner_iota == hot_second)
    offsets = jax.random.randint(sub_keys[3], (GROUP_SIZE, GROUP_SIZE), 0, rows_owner)
    offsets = jnp.where(hot_owner[None, :], 0, offsets)
    window_cols = (offsets[:, :, None] + jnp.arange(DISTINCT)[None, None, :]) % rows_owner
    request_rows = owner_perm[owner_iota[None, :, None], window_cols]
    cover_rank = jax.vmap(lambda one_key: jax.random.permutation(one_key, sel_dev))(jax.random.split(sub_keys[4], GROUP_SIZE))
    hot_pick = jax.random.randint(sub_keys[5], (GROUP_SIZE, sel_dev), 0, 2) == 0
    hot_side = jnp.where(jax.random.randint(sub_keys[6], (GROUP_SIZE, sel_dev), 0, 2) == 0, hot_first, hot_second)
    hot_slot = hot_side * DISTINCT + jax.random.randint(sub_keys[7], (GROUP_SIZE, sel_dev), 0, hot_slots)
    cold_slot = jax.random.randint(sub_keys[8], (GROUP_SIZE, sel_dev), 0, slots_dev)
    slot_ids = jnp.where(cover_rank < slots_dev, cover_rank, jnp.where(hot_pick, hot_slot, cold_slot))
    slot_ids = slot_ids.reshape(GROUP_SIZE * TOKENS_DEV, NUM_HEADS, TOP_K).astype(jnp.int32)
    return slot_ids, request_rows.astype(jnp.int32)


def setup_inputs(seed: int = 0, part: int = 0) -> dict:
    part_key = jax.random.fold_in(jax.random.key(seed), part)
    key_tok, key_grad, key_gate, key_route = jax.random.split(part_key, 4)
    key_up, key_down = jax.random.split(jax.random.key(seed + 1), 2)
    n_tok = GROUP_SIZE * TOKENS_DEV
    sel_tok = NUM_HEADS * TOP_K
    tokens = jax.random.normal(key_tok, (n_tok, MODEL_DIM), jnp.float32)
    grad_out = jax.random.normal(key_grad, (n_tok, MODEL_DIM), jnp.float32)
    gate_vals = jax.random.uniform(key_gate, (n_tok, NUM_HEADS, TOP_K), jnp.float32, 0.25, 1.75)
    table_up = jax.random.normal(key_up, (EXPERTS, MODEL_DIM), jnp.float32) * MODEL_DIM ** -0.5
    table_down = jax.random.normal(key_down, (EXPERTS, MODEL_DIM), jnp.float32) * sel_tok ** -0.5
    slot_ids, request_rows = draw_routing(key_route)
    return dict(tokens=tokens.astype(jnp.bfloat16), slot_ids=slot_ids, request_rows=request_rows, gate_vals=gate_vals, grad_out=grad_out.astype(jnp.bfloat16), table_up=table_up.astype(jnp.bfloat16), table_down=table_down.astype(jnp.bfloat16))


def gelu_pair(pre_act):
    normal_cdf = 0.5 * (1.0 + lax.erf(pre_act * (2.0 ** -0.5)))
    normal_pdf = jnp.exp(-0.5 * pre_act * pre_act) * ((2.0 * math.pi) ** -0.5)
    return pre_act * normal_cdf, normal_cdf + pre_act * normal_pdf


def reference(tokens, slot_ids, request_rows, gate_vals, grad_out, table_up, table_down):
    n_tok = GROUP_SIZE * TOKENS_DEV
    sel_tok = NUM_HEADS * TOP_K
    rows_owner = EXPERTS // GROUP_SIZE
    slot_flat = slot_ids.reshape(n_tok, sel_tok)
    dev_idx = jnp.arange(n_tok)[:, None] // TOKENS_DEV
    owner_idx = slot_flat // DISTINCT
    expert_ids = owner_idx * rows_owner + request_rows[dev_idx, owner_idx, slot_flat % DISTINCT]
    cap_tokens = max(1, 2 ** 23 // (sel_tok * MODEL_DIM))
    block_tok = math.gcd(n_tok, 2 ** int(math.log2(cap_tokens)))
    n_blocks = n_tok // block_tok

    def scan_step(acc_pair, block_in):
        acc_up, acc_down = acc_pair
        x_blk, id_blk, gate_blk, dy_blk = block_in
        x_wide = x_blk.astype(jnp.float32)
        dy_wide = dy_blk.astype(jnp.float32)
        up_rows = table_up[id_blk].astype(jnp.float32)
        down_rows = table_down[id_blk].astype(jnp.float32)
        pre_act = jnp.einsum('bsd,bd->bs', up_rows, x_wide)
        act_val, slope_val = gelu_pair(pre_act)
        w_out = (gate_blk * act_val).astype(jnp.bfloat16).astype(jnp.float32)
        y_blk = jnp.einsum('bs,bsd->bd', w_out, down_rows)
        back_dot = jnp.einsum('bsd,bd->bs', down_rows, dy_wide)
        coef_val = (gate_blk * slope_val * back_dot).astype(jnp.bfloat16).astype(jnp.float32)
        dx_blk = jnp.einsum('bs,bsd->bd', coef_val, up_rows)
        flat_ids = id_blk.reshape(-1)
        acc_up = acc_up.at[flat_ids].add((coef_val[:, :, None] * x_wide[:, None, :]).reshape(-1, MODEL_DIM))
        acc_down = acc_down.at[flat_ids].add((w_out[:, :, None] * dy_wide[:, None, :]).reshape(-1, MODEL_DIM))
        return (acc_up, acc_down), (y_blk, dx_blk)

    zero_acc = jnp.zeros((EXPERTS, MODEL_DIM), jnp.float32)
    blocks_in = (tokens.reshape(n_blocks, block_tok, MODEL_DIM), expert_ids.reshape(n_blocks, block_tok, sel_tok), gate_vals.reshape(n_blocks, block_tok, sel_tok), grad_out.reshape(n_blocks, block_tok, MODEL_DIM))
    (acc_up, acc_down), (y_all, dx_all) = lax.scan(scan_step, (zero_acc, zero_acc), blocks_in)
    out_tokens = y_all.reshape(n_tok, MODEL_DIM).astype(jnp.bfloat16)
    grad_tokens = dx_all.reshape(n_tok, MODEL_DIM).astype(jnp.bfloat16)
    return (out_tokens, grad_tokens, acc_up.astype(jnp.bfloat16), acc_down.astype(jnp.bfloat16))
```

```python
import functools
import math
import jax
import jax.numpy as jnp
from jax import lax
from jax.experimental import pallas as pl
from jax.experimental.pallas import tpu as pltpu
from jax.sharding import PartitionSpec as P


CORE, ZTOK, ZTAB = 1, 32, 96
N_EP, ROWS, REQ = 128, 128, 64
N_SET = 4
N_OWN = 32
N_GRP = N_OWN // 4
N_HI = N_OWN * REQ // 128
F32, BF16 = jnp.float32, jnp.bfloat16
NT = (((1,), (1,)), ((), ()))

ERF_NUM = (0.00022905065861350646, 0.0034082910107109506, 0.050955695062380861, 0.18520832239976145, 1.128379143519084)
ERF_DEN = (-1.1791602954361697e-7, 0.000023547966471313185, 0.0010179625278914885, 0.014070470171167667, 0.11098505178285362, 0.49746925110067538, 1.0)


def poly(x, coefs):
    acc = jnp.full_like(x, coefs[0])
    for one in coefs[1:]:
        acc = acc * x + one
    return acc


def gelu_pair(pre_act):
    arg = jnp.clip(pre_act * (2.0 ** -0.5), -3.832506856900711, 3.832506856900711)
    arg2 = arg * arg
    normal_cdf = 0.5 + 0.5 * (arg * poly(arg2, ERF_NUM) / poly(arg2, ERF_DEN))
    normal_pdf = jnp.exp(-0.5 * pre_act * pre_act) * ((2.0 * math.pi) ** -0.5)
    return pre_act * normal_cdf, normal_cdf + pre_act * normal_pdf


def dot(a, b, dims=(((1,), (0,)), ((), ()))):
    return lax.dot_general(a, b, dims, preferred_element_type=F32)


def gate_kernel(hi_ref, lo_ref, g1_ref, g2_ref, g3_ref, out_ref, flat):
    tok_blk = hi_ref.shape[0]
    row_iota = lax.broadcasted_iota(jnp.int32, (16, 128), 0).astype(F32)
    iotas = [(row_iota + 16.0 * k).astype(BF16) for k in range(8)]

    def spread(ref, t):
        return jnp.broadcast_to(ref[pl.ds(t, 1), :], (16, 128)).astype(BF16)

    def one_token(t):
        zero = jnp.zeros((16, 128), BF16)
        one = jnp.ones((16, 128), BF16)
        hit = spread(hi_ref, t) == iotas[0]
        lhs = jnp.concatenate([jnp.where(hit, spread(ref, t), zero) for ref in (g1_ref, g2_ref, g3_ref)], axis=0)
        lo_row = spread(lo_ref, t)
        rhs = jnp.concatenate([jnp.where(lo_row == one_iota, one, zero) for one_iota in iotas], axis=0)
        res = dot(lhs, rhs, NT)
        flat[pl.ds(t, N_HI, stride=tok_blk), :] = (res[32:48] + res[16:32]) + res[:16]

    def body(step, carry):
        for k in range(8):
            one_token(step * 8 + k)
        return carry

    lax.fori_loop(0, tok_blk // 8, body, 0)
    for h in range(N_HI):
        out_ref[h] = flat[pl.ds(h * tok_blk, tok_blk), :]


def gate_matrix(hi, lo, g1, g2, g3):
    n_tok = hi.shape[0]
    tok_blk = min(128, n_tok)
    spec = pl.BlockSpec((tok_blk, 128), lambda i: (i, 0))
    return pl.pallas_call(
        gate_kernel,
        grid=(n_tok // tok_blk,),
        in_specs=[spec] * 5,
        out_specs=pl.BlockSpec((N_HI, tok_blk, 128), lambda i: (0, i, 0)),
        out_shape=jax.ShapeDtypeStruct((N_HI, n_tok, 128), F32),
        scratch_shapes=[pltpu.VMEM((N_HI * tok_blk, 128), F32)],
        compiler_params=pltpu.CompilerParams(vmem_limit_bytes=60 * 2 ** 20),
        cost_estimate=pl.CostEstimate(flops=n_tok * 8 * 2 ** 20, bytes_accessed=n_tok * 2 ** 13, transcendentals=0),
        name="gate_matrix",
    )(hi, lo, g1, g2, g3)


def first_kernel(n_tok, tok_chunk, u_ref, p_ref, pt_ref, gl_ref, gr_ref, *refs):
    xd_refs = refs[:N_SET]
    uc_ref, w_ref, s_ref, dv_ref, wrt = refs[N_SET:]
    for s in range(N_SET):
        g_ref = gl_ref if s < 2 else gr_ref
        g_base = (s % 2) * n_tok
        for i in range(2):
            uc_ref[0, s, i * 128:(i + 1) * 128, :] = dot(p_ref[0, s, i], u_ref[i * 256:(i + 1) * 256, :]).astype(BF16)
        for t0 in range(0, n_tok, tok_chunk):
            pre_act = dot(xd_refs[s][t0:t0 + tok_chunk, :], uc_ref[0, s], NT)
            row0 = s * n_tok + t0
            for i in range(2):
                gate = g_ref[i, g_base + t0:g_base + t0 + tok_chunk, :]
                act, slope = gelu_pair(pre_act[:, i * 128:(i + 1) * 128])
                used = gate > 0.0
                w_ref[row0:row0 + tok_chunk, i * 128:(i + 1) * 128] = jnp.where(used, gate * act, 0.0).astype(BF16)
                s_ref[row0:row0 + tok_chunk, i * 128:(i + 1) * 128] = jnp.where(used, gate * slope, 0.0)
        for i in range(2):
            wrt[i * 256:(i + 1) * 256, s * n_tok:(s + 1) * n_tok] = dot(pt_ref[0, s, i], w_ref[s * n_tok:(s + 1) * n_tok, i * 128:(i + 1) * 128], NT).astype(BF16)
    dy_all = jnp.concatenate([ref[n_tok:, :] for ref in xd_refs], axis=0)
    dv_ref[...] = dot(wrt[...], dy_all).astype(BF16)


def whole(arr):
    return pl.BlockSpec(arr.shape, lambda g: (0,) * arr.ndim, pipeline_mode=pl.Buffered(1))


def first_pass(u_all, p_hot, pt_hot, g_loc, g_rem, xds):
    n_tok, width = xds[0].shape[0] // 2, xds[0].shape[1]
    all_tok = N_SET * n_tok
    flops = 2 * N_GRP * N_SET * (256 * 256 * width + n_tok * width * 256 + n_tok * 128 * 512 + n_tok * 512 * width)
    return pl.pallas_call(
        functools.partial(first_kernel, n_tok, min(128, n_tok)),
        grid=(N_GRP,),
        in_specs=[
            pl.BlockSpec((512, width), lambda g: (g, 0)),
            pl.BlockSpec((1, N_SET, 2, 128, 256), lambda g: (g, 0, 0, 0, 0)),
            pl.BlockSpec((1, N_SET, 2, 256, 128), lambda g: (g, 0, 0, 0, 0)),
            pl.BlockSpec((2, 2 * n_tok, 128), lambda g: (g, 0, 0)),
            pl.BlockSpec((2, 2 * n_tok, 128), lambda g: (g, 0, 0)),
        ] + [whole(xd) for xd in xds],
        out_specs=[
            pl.BlockSpec((1, N_SET, 256, width), lambda g: (g, 0, 0, 0)),
            pl.BlockSpec((all_tok, 256), lambda g: (0, g)),
            pl.BlockSpec((all_tok, 256), lambda g: (0, g)),
            pl.BlockSpec((512, width), lambda g: (g, 0)),
        ],
        out_shape=[
            jax.ShapeDtypeStruct((N_GRP, N_SET, 256, width), BF16),
            jax.ShapeDtypeStruct((all_tok, N_GRP * 256), BF16),
            jax.ShapeDtypeStruct((all_tok, N_GRP * 256), F32),
            jax.ShapeDtypeStruct((N_GRP * 512, width), BF16),
        ],
        scratch_shapes=[pltpu.VMEM((512, all_tok), BF16)],
        compiler_params=pltpu.CompilerParams(vmem_limit_bytes=60 * 2 ** 20),
        cost_estimate=pl.CostEstimate(flops=flops, bytes_accessed=76 * 2 ** 20, transcendentals=all_tok * N_GRP * 256),
        name="first_pass",
    )(u_all, p_hot, pt_hot, g_loc, g_rem, *xds)


def down_kernel(n_tok, v_ref, p_ref, w_ref, vc_ref, y_ref):
    first = pl.program_id(0) == 0
    for s in range(N_SET):
        for i in range(2):
            vc_ref[0, s, i * 128:(i + 1) * 128, :] = dot(p_ref[0, s, i], v_ref[i * 256:(i + 1) * 256, :]).astype(BF16)

    @pl.when(first)
    def _():
        for s in range(N_SET):
            y_ref[s * n_tok:(s + 1) * n_tok, :] = dot(w_ref[s * n_tok:(s + 1) * n_tok, :], vc_ref[0, s])

    @pl.when(jnp.logical_not(first))
    def _():
        for s in range(N_SET):
            y_ref[s * n_tok:(s + 1) * n_tok, :] += dot(w_ref[s * n_tok:(s + 1) * n_tok, :], vc_ref[0, s])


def down_pass(v_all, p_hot, w_all):
    width = v_all.shape[1]
    all_tok = w_all.shape[0]
    n_tok = all_tok // N_SET
    flops = 2 * N_GRP * N_SET * (256 * 256 * width + n_tok * width * 256)
    return pl.pallas_call(
        functools.partial(down_kernel, n_tok),
        grid=(N_GRP,),
        in_specs=[
            pl.BlockSpec((512, width), lambda g: (g, 0)),
            pl.BlockSpec((1, N_SET, 2, 128, 256), lambda g: (g, 0, 0, 0, 0)),
            pl.BlockSpec((all_tok, 256), lambda g: (0, g)),
        ],
        out_specs=[
            pl.BlockSpec((1, N_SET, 256, width), lambda g: (g, 0, 0, 0)),
            pl.BlockSpec((all_tok, width), lambda g: (0, 0)),
        ],
        out_shape=[
            jax.ShapeDtypeStruct((N_GRP, N_SET, 256, width), BF16),
            jax.ShapeDtypeStruct((all_tok, width), F32),
        ],
        compiler_params=pltpu.CompilerParams(vmem_limit_bytes=60 * 2 ** 20),
        cost_estimate=pl.CostEstimate(flops=flops, bytes_accessed=44 * 2 ** 20, transcendentals=0),
        name="down_pass",
    )(v_all, p_hot, w_all)


def second_kernel(n_tok, tok_chunk, vc_ref, pt_ref, s_ref, *refs):
    xd_refs = refs[:N_SET]
    c_ref, du_ref, crt = refs[N_SET:]
    for s in range(N_SET):
        for t0 in range(0, n_tok, tok_chunk):
            back = dot(xd_refs[s][n_tok + t0:n_tok + t0 + tok_chunk, :], vc_ref[0, s], NT)
            row0 = s * n_tok + t0
            slope = s_ref[row0:row0 + tok_chunk, :]
            c_ref[row0:row0 + tok_chunk, :] = jnp.where(slope == 0.0, 0.0, slope * back).astype(BF16)
        for i in range(2):
            crt[i * 256:(i + 1) * 256, s * n_tok:(s + 1) * n_tok] = dot(pt_ref[0, s, i], c_ref[s * n_tok:(s + 1) * n_tok, i * 128:(i + 1) * 128], NT).astype(BF16)
    x_all = jnp.concatenate([ref[:n_tok, :] for ref in xd_refs], axis=0)
    du_ref[...] = dot(crt[...], x_all).astype(BF16)


def second_pass(vc, pt_hot, slopes, xds):
    n_tok, width = xds[0].shape[0] // 2, xds[0].shape[1]
    all_tok = N_SET * n_tok
    flops = 2 * N_GRP * N_SET * (n_tok * width * 256 + n_tok * 128 * 512 + n_tok * 512 * width)
    return pl.pallas_call(
        functools.partial(second_kernel, n_tok, min(128, n_tok)),
        grid=(N_GRP,),
        in_specs=[
            pl.BlockSpec((1, N_SET, 256, width), lambda g: (g, 0, 0, 0)),
            pl.BlockSpec((1, N_SET, 2, 256, 128), lambda g: (g, 0, 0, 0, 0)),
            pl.BlockSpec((all_tok, 256), lambda g: (0, g)),
        ] + [whole(xd) for xd in xds],
        out_specs=[
            pl.BlockSpec((all_tok, 256), lambda g: (0, g)),
            pl.BlockSpec((512, width), lambda g: (g, 0)),
        ],
        out_shape=[
            jax.ShapeDtypeStruct((all_tok, N_GRP * 256), BF16),
            jax.ShapeDtypeStruct((N_GRP * 512, width), BF16),
        ],
        scratch_shapes=[pltpu.VMEM((512, all_tok), BF16)],
        compiler_params=pltpu.CompilerParams(vmem_limit_bytes=60 * 2 ** 20),
        cost_estimate=pl.CostEstimate(flops=flops, bytes_accessed=58 * 2 ** 20, transcendentals=0),
        name="second_pass",
    )(vc, pt_hot, slopes, *xds)


def token_grad_kernel(c_ref, uc_ref, dx_ref):
    width = uc_ref.shape[-1]
    dx_ref[...] = dot(c_ref[...], uc_ref[...].reshape(N_GRP * 256, width))


def token_grad(c_all, uc, first_set):
    width = uc.shape[-1]
    n_tok = c_all.shape[0] // N_SET
    flops = 2 * 2 * n_tok * N_GRP * 256 * width
    return pl.pallas_call(
        token_grad_kernel,
        grid=(2,),
        in_specs=[
            pl.BlockSpec((n_tok, N_GRP * 256), lambda i: (first_set + i, 0)),
            pl.BlockSpec((N_GRP, 1, 256, width), lambda i: (0, first_set + i, 0, 0)),
        ],
        out_specs=pl.BlockSpec((n_tok, width), lambda i: (i, 0)),
        out_shape=jax.ShapeDtypeStruct((2 * n_tok, width), F32),
        compiler_params=pltpu.CompilerParams(vmem_limit_bytes=60 * 2 ** 20),
        cost_estimate=pl.CostEstimate(flops=flops, bytes_accessed=16 * 2 ** 20, transcendentals=0),
        name="token_grad",
    )(c_all, uc)


def hot_tables(req_sets, core, zgrp):
    yx = jnp.arange(16)[:, None]
    z_of = jnp.where(zgrp == 0, jnp.array([0, 3]), jnp.array([1, 2]))[None, :]
    owners = ((z_of * 16 + yx) * 2 + core).reshape(N_OWN)
    req = jnp.stack([one[owners] for one in req_sets], axis=1)
    req = req.reshape(N_GRP, 2, 2, N_SET, REQ).transpose(0, 3, 1, 2, 4)
    row = (req + ROWS * jnp.arange(2)[:, None]).reshape(N_GRP, N_SET, 2, 2 * REQ)
    ids = jnp.arange(2 * ROWS)
    p_hot = (row[..., :, None] == ids).astype(BF16)
    pt_hot = (row[..., None, :] == ids[:, None]).astype(BF16)
    return p_hot, pt_hot


def gate_inputs(slots, gates, core, zgrp):
    slot = slots.astype(jnp.int32)
    owner = slot // REQ
    z_of = owner // 32
    here = ((owner % 2) == core) & ((((z_of + 1) // 2) % 2) == zgrp)
    local = (((owner // 2) % 16) * 2 + z_of // 2) * REQ + slot % REQ
    hi = jnp.where(here, local // 128, 255).astype(F32)
    lo = (local % 128).astype(F32)
    g1 = lax.reduce_precision(gates, 8, 7)
    g2 = lax.reduce_precision(gates - g1, 8, 7)
    g3 = lax.reduce_precision(gates - g1 - g2, 8, 7)
    return hi, lo, g1, g2, g3


def solution(mesh):
    tok_spec = P(('dp', 'ep'))
    table_spec = P('ep')
    plane = [[z * 32 + yx * 2 + c for yx in range(16)] for z in range(4) for c in range(2)]

    def swap(arr, mask):
        return lax.ppermute(arr, 'ep', [(i, i ^ mask) for i in range(N_EP)])

    def per_device(tokens, slot_ids, request_rows, gate_vals, grad_out, up_local, down_local):
        n_tok, width = tokens.shape
        n_sel = slot_ids.shape[1] * slot_ids.shape[2]
        index = lax.axis_index('ep')
        core, z_me = index % 2, index // 32
        zgrp = ((z_me + 1) // 2) % 2

        def table_rows(local):
            other = swap(local, ZTAB)
            both = jnp.where(z_me < 2, jnp.concatenate([local, other]), jnp.concatenate([other, local]))
            return lax.all_gather(both, 'ep', axis=0, tiled=True, axis_index_groups=plane)

        def grad_rows(part):
            mine = lax.psum_scatter(part, 'ep', scatter_dimension=0, tiled=True, axis_index_groups=plane)
            keep = lax.dynamic_slice_in_dim(mine, (z_me // 2) * ROWS, ROWS)
            give = lax.dynamic_slice_in_dim(mine, (1 - z_me // 2) * ROWS, ROWS)
            return (keep.astype(F32) + swap(give, ZTAB).astype(F32)).astype(BF16)

        def collect(local_part, remote_part):
            from_core = swap(local_part[n_tok:], CORE)
            for_z = remote_part[:n_tok] + swap(remote_part[n_tok:], CORE)
            return (local_part[:n_tok] + from_core + swap(for_z, ZTOK)).astype(BF16)

        n_req = request_rows.shape[1] * request_rows.shape[2] // n_sel
        meta0 = jnp.concatenate([slot_ids.reshape(n_tok, n_sel).astype(F32), gate_vals.reshape(n_tok, n_sel), request_rows.reshape(n_req, n_sel).astype(F32)])
        xd0 = jnp.concatenate([tokens, grad_out])
        meta2 = swap(meta0, ZTOK)
        meta1 = swap(meta0, CORE)
        meta3 = swap(meta2, CORE)
        u_all = table_rows(up_local)
        v_all = table_rows(down_local)
        xd2 = swap(xd0, ZTOK)
        xd1 = swap(xd0, CORE)
        xd3 = swap(xd2, CORE)
        metas = (meta0, meta1, meta2, meta3)
        xds = (xd0, xd1, xd2, xd3)
        p_hot, pt_hot = hot_tables([m[2 * n_tok:].reshape(N_EP, REQ).astype(jnp.int32) for m in metas], core, zgrp)

        def gates_of(ma, mb):
            return gate_matrix(*gate_inputs(jnp.concatenate([ma[:n_tok], mb[:n_tok]]), jnp.concatenate([ma[n_tok:2 * n_tok], mb[n_tok:2 * n_tok]]), core, zgrp))

        g_loc = gates_of(meta0, meta1)
        g_rem = gates_of(meta2, meta3)
        uc, w_all, slopes, dv_part = first_pass(u_all, p_hot, pt_hot, g_loc, g_rem, xds)
        vc, y_part = down_pass(v_all, p_hot, w_all)
        c_all, du_part = second_pass(vc, pt_hot, slopes, xds)
        dx_rem = token_grad(c_all, uc, 2)
        dx_loc = token_grad(c_all, uc, 0)
        y = collect(y_part[:2 * n_tok], y_part[2 * n_tok:])
        grad_down = grad_rows(dv_part)
        grad_up = grad_rows(du_part)
        dx = collect(dx_loc, dx_rem)
        return y, dx, grad_up, grad_down

    return jax.shard_map(per_device, mesh=mesh, in_specs=(tok_spec, tok_spec, tok_spec, tok_spec, tok_spec, table_spec, table_spec), out_specs=(tok_spec, tok_spec, tok_spec, tok_spec), check_vma=False)
```

```python
import functools
import math
import jax
import jax.numpy as jnp
from jax import lax
from jax.experimental import pallas as pl
from jax.experimental.pallas import tpu as pltpu
from jax.sharding import PartitionSpec as P


CORE, ZTOK, ZTAB = 1, 32, 96
N_EP, ROWS, REQ = 128, 128, 64
N_SET = 4
N_OWN = 32
N_GRP = N_OWN // 4
N_HI = N_OWN * REQ // 128
F32, BF16 = jnp.float32, jnp.bfloat16
NT = (((1,), (1,)), ((), ()))


def gelu_pair(pre_act):
    normal_cdf = 0.5 * (1.0 + lax.erf(pre_act * (2.0 ** -0.5)))
    normal_pdf = jnp.exp(-0.5 * pre_act * pre_act) * ((2.0 * math.pi) ** -0.5)
    return pre_act * normal_cdf, normal_cdf + pre_act * normal_pdf


def dot(a, b, dims=(((1,), (0,)), ((), ()))):
    return lax.dot_general(a, b, dims, preferred_element_type=F32)


def gate_kernel(ctl_ref, slot_ref, gate_ref, out_ref, hi_ref, lo_ref, g1_ref, g2_ref, g3_ref):
    n_tok = slot_ref.shape[0]
    slot = slot_ref[...].astype(jnp.int32)
    owner = slot >> 6
    z_of = owner >> 5
    here = ((owner & 1) == ctl_ref[0]) & ((((z_of + 1) >> 1) & 1) == ctl_ref[1])
    local = ((((owner >> 1) & 15) * 2 + (z_of >> 1)) << 6) + (slot & 63)
    hi_ref[...] = jnp.where(here, local >> 7, 255).astype(F32)
    lo_ref[...] = (local & 127).astype(F32)
    gate = gate_ref[...]
    g1 = gate.astype(BF16).astype(F32)
    g2 = (gate - g1).astype(BF16).astype(F32)
    g1_ref[...] = g1
    g2_ref[...] = g2
    g3_ref[...] = (gate - g1) - g2
    row_iota = lax.broadcasted_iota(jnp.int32, (16, 128), 0).astype(F32)
    iotas = [(row_iota + 16.0 * k).astype(BF16) for k in range(8)]
    out_flat = out_ref.reshape(n_tok * N_HI, 128)

    def spread(ref, t):
        return jnp.broadcast_to(ref[pl.ds(t, 1), :], (16, 128)).astype(BF16)

    def sides(t):
        hit = spread(hi_ref, t) == iotas[0]
        lhs = jnp.concatenate([jnp.where(hit, spread(ref, t), jnp.zeros((16, 128), BF16)) for ref in (g1_ref, g2_ref, g3_ref)], axis=0)
        lo_row = spread(lo_ref, t)
        rhs = jnp.concatenate([jnp.where(lo_row == one_iota, jnp.ones((16, 128), BF16), jnp.zeros((16, 128), BF16)) for one_iota in iotas], axis=0)
        return lhs, rhs

    def two_tokens(t):
        lhs_a, rhs_a = sides(t)
        lhs_b, rhs_b = sides(t + 1)
        empty = jnp.zeros_like(lhs_a)
        lhs = jnp.concatenate([jnp.concatenate([lhs_a, empty], axis=1), jnp.concatenate([empty, lhs_b], axis=1)], axis=0)
        res = dot(lhs, jnp.concatenate([rhs_a, rhs_b], axis=1), NT)
        return (res[32:48] + res[16:32]) + res[:16], (res[80:96] + res[64:80]) + res[48:64]

    def body(step, carry):
        for k in range(0, tok_step, 2):
            row_a, row_b = two_tokens(step * tok_step + k)
            base = (step * (tok_step // 8) + k // 8) * (8 * N_HI) + k % 8
            out_flat[pl.ds(base, N_HI, stride=8), :] = row_a
            out_flat[pl.ds(base + 1, N_HI, stride=8), :] = row_b
        return carry

    tok_step = min(64, n_tok)
    lax.fori_loop(0, n_tok // tok_step, body, 0)


def gate_matrix(ctl, meta, n_tok):
    tok_blk = min(256, n_tok)
    n_blk = n_tok // tok_blk
    return pl.pallas_call(
        gate_kernel,
        grid=(n_blk,),
        in_specs=[
            pl.BlockSpec(memory_space=pltpu.SMEM),
            pl.BlockSpec((tok_blk, 128), lambda i: (i, 0)),
            pl.BlockSpec((tok_blk, 128), lambda i: (i + n_blk, 0)),
        ],
        out_specs=pl.BlockSpec((tok_blk // 8, N_HI, 8, 128), lambda i: (i, 0, 0, 0)),
        out_shape=jax.ShapeDtypeStruct((n_tok // 8, N_HI, 8, 128), F32),
        scratch_shapes=[pltpu.VMEM((tok_blk, 128), F32)] * 5,
        compiler_params=pltpu.CompilerParams(vmem_limit_bytes=32 * 2 ** 20),
        cost_estimate=pl.CostEstimate(flops=n_tok * 12 * 2 ** 20, bytes_accessed=n_tok * 9216, transcendentals=0),
        name="gate_matrix",
    )(ctl, meta, meta)


def pick_rows(p_ref, table_ref, out_ref):
    for i in range(2):
        rows = dot(p_ref[0, i], table_ref[i * 256:(i + 1) * 256, :]).astype(BF16)
        for s in range(N_SET):
            out_ref[0, s, i * 128:(i + 1) * 128, :] = rows[s * 128:(s + 1) * 128]


def halves(n_tok):
    half = max(n_tok // 2, 16)
    return [slice(t, t + half) for t in range(0, n_tok, half)]


def first_kernel(n_tok, u_ref, p_ref, pt_ref, *refs):
    g_refs, xd_refs = refs[:N_SET], refs[N_SET:2 * N_SET]
    uc_ref, w_ref, s_ref, dv_ref, wrt, pre = refs[2 * N_SET:]
    tok_chunk = min(64, n_tok)

    def front(s):
        for part in halves(n_tok):
            pre[s, part, :] = dot(xd_refs[s][part, :], uc_ref[0, s], NT)

    def back(s):
        for t0 in range(0, n_tok, tok_chunk):
            row0 = s * n_tok + t0
            for i in range(2):
                gate = g_refs[s][t0 // 8:(t0 + tok_chunk) // 8, i].reshape(tok_chunk, 128)
                act, slope = gelu_pair(pre[s, t0:t0 + tok_chunk, i * 128:(i + 1) * 128])
                used = gate > 0.0
                w_ref[row0:row0 + tok_chunk, i * 128:(i + 1) * 128] = jnp.where(used, gate * act, 0.0).astype(BF16)
                s_ref[row0:row0 + tok_chunk, i * 128:(i + 1) * 128] = jnp.where(used, gate * slope, 0.0)
        for i in range(2):
            wrt[i * 256:(i + 1) * 256, s * n_tok:(s + 1) * n_tok] = dot(pt_ref[0, s, i], w_ref[s * n_tok:(s + 1) * n_tok, i * 128:(i + 1) * 128], NT).astype(BF16)

    pick_rows(p_ref, u_ref, uc_ref)
    front(0)
    for s in range(1, N_SET):
        front(s)
        back(s - 1)
    back(N_SET - 1)
    dy_all = jnp.concatenate([ref[n_tok:, :] for ref in xd_refs], axis=0)
    dv_ref[...] = dot(wrt[...], dy_all).astype(BF16)


def whole(arr):
    return pl.BlockSpec(arr.shape, lambda g: (0,) * arr.ndim, pipeline_mode=pl.Buffered(1))


def first_pass(u_all, p_hot, pt_hot, gates, xds):
    n_tok, width = xds[0].shape[0] // 2, xds[0].shape[1]
    all_tok = N_SET * n_tok
    flops = 2 * N_GRP * N_SET * (256 * 256 * width + n_tok * width * 256 + n_tok * 128 * 512 + n_tok * 512 * width)
    return pl.pallas_call(
        functools.partial(first_kernel, n_tok),
        grid=(N_GRP,),
        in_specs=[
            pl.BlockSpec((512, width), lambda g: (g, 0)),
            pl.BlockSpec((1, 2, N_SET * 128, 256), lambda g: (g, 0, 0, 0)),
            pl.BlockSpec((1, N_SET, 2, 256, 128), lambda g: (g, 0, 0, 0, 0)),
        ] + [pl.BlockSpec((n_tok // 8, 2, 8, 128), lambda g: (0, g, 0, 0))] * N_SET + [whole(xd) for xd in xds],
        out_specs=[
            pl.BlockSpec((1, N_SET, 256, width), lambda g: (g, 0, 0, 0)),
            pl.BlockSpec((all_tok, 256), lambda g: (0, g)),
            pl.BlockSpec((all_tok, 256), lambda g: (0, g)),
            pl.BlockSpec((512, width), lambda g: (g, 0)),
        ],
        out_shape=[
            jax.ShapeDtypeStruct((N_GRP, N_SET, 256, width), BF16),
            jax.ShapeDtypeStruct((all_tok, N_GRP * 256), BF16),
            jax.ShapeDtypeStruct((all_tok, N_GRP * 256), F32),
            jax.ShapeDtypeStruct((N_GRP * 512, width), BF16),
        ],
        scratch_shapes=[pltpu.VMEM((512, all_tok), BF16), pltpu.VMEM((N_SET, n_tok, 256), F32)],
        compiler_params=pltpu.CompilerParams(vmem_limit_bytes=60 * 2 ** 20),
        cost_estimate=pl.CostEstimate(flops=flops, bytes_accessed=76 * 2 ** 20, transcendentals=all_tok * N_GRP * 256),
        name="first_pass",
    )(u_all, p_hot, pt_hot, *gates, *xds)


def down_kernel(n_tok, v_ref, p_ref, w_ref, vc_ref, y_ref):
    @pl.when(pl.program_id(0) == 0)
    def _():
        y_ref[...] = jnp.zeros_like(y_ref)

    pick_rows(p_ref, v_ref, vc_ref)
    for s in range(N_SET):
        y_ref[s * n_tok:(s + 1) * n_tok, :] += dot(w_ref[s * n_tok:(s + 1) * n_tok, :], vc_ref[0, s])


def down_pass(v_all, p_hot, w_all):
    width = v_all.shape[1]
    all_tok = w_all.shape[0]
    n_tok = all_tok // N_SET
    flops = 2 * N_GRP * N_SET * (256 * 256 * width + n_tok * width * 256)
    return pl.pallas_call(
        functools.partial(down_kernel, n_tok),
        grid=(N_GRP,),
        in_specs=[
            pl.BlockSpec((512, width), lambda g: (g, 0)),
            pl.BlockSpec((1, 2, N_SET * 128, 256), lambda g: (g, 0, 0, 0)),
            pl.BlockSpec((all_tok, 256), lambda g: (0, g)),
        ],
        out_specs=[
            pl.BlockSpec((1, N_SET, 256, width), lambda g: (g, 0, 0, 0)),
            pl.BlockSpec((all_tok, width), lambda g: (0, 0)),
        ],
        out_shape=[
            jax.ShapeDtypeStruct((N_GRP, N_SET, 256, width), BF16),
            jax.ShapeDtypeStruct((all_tok, width), F32),
        ],
        compiler_params=pltpu.CompilerParams(vmem_limit_bytes=60 * 2 ** 20),
        cost_estimate=pl.CostEstimate(flops=flops, bytes_accessed=44 * 2 ** 20, transcendentals=0),
        name="down_pass",
    )(v_all, p_hot, w_all)


def second_kernel(n_tok, vc_ref, pt_ref, s_ref, *refs):
    xd_refs = refs[:N_SET]
    c_ref, du_ref, crt = refs[N_SET:]

    def front(s):
        for part in halves(n_tok):
            rows = slice(s * n_tok + part.start, s * n_tok + part.stop)
            back = dot(xd_refs[s][n_tok + part.start:n_tok + part.stop, :], vc_ref[0, s], NT)
            slope = s_ref[rows, :]
            c_ref[rows, :] = jnp.where(slope == 0.0, 0.0, slope * back).astype(BF16)

    def back(s):
        rows = slice(s * n_tok, (s + 1) * n_tok)
        for i in range(2):
            crt[i * 256:(i + 1) * 256, rows] = dot(pt_ref[0, s, i], c_ref[rows, i * 128:(i + 1) * 128], NT).astype(BF16)

    front(0)
    for s in range(1, N_SET):
        front(s)
        back(s - 1)
    back(N_SET - 1)
    x_all = jnp.concatenate([ref[:n_tok, :] for ref in xd_refs], axis=0)
    du_ref[...] = dot(crt[...], x_all).astype(BF16)


def second_pass(vc, pt_hot, slopes, xds):
    n_tok, width = xds[0].shape[0] // 2, xds[0].shape[1]
    all_tok = N_SET * n_tok
    flops = 2 * N_GRP * N_SET * (n_tok * width * 256 + n_tok * 128 * 512 + n_tok * 512 * width)
    return pl.pallas_call(
        functools.partial(second_kernel, n_tok),
        grid=(N_GRP,),
        in_specs=[
            pl.BlockSpec((1, N_SET, 256, width), lambda g: (g, 0, 0, 0)),
            pl.BlockSpec((1, N_SET, 2, 256, 128), lambda g: (g, 0, 0, 0, 0)),
            pl.BlockSpec((all_tok, 256), lambda g: (0, g)),
        ] + [whole(xd) for xd in xds],
        out_specs=[
            pl.BlockSpec((all_tok, 256), lambda g: (0, g)),
            pl.BlockSpec((512, width), lambda g: (g, 0)),
        ],
        out_shape=[
            jax.ShapeDtypeStruct((all_tok, N_GRP * 256), BF16),
            jax.ShapeDtypeStruct((N_GRP * 512, width), BF16),
        ],
        scratch_shapes=[pltpu.VMEM((512, all_tok), BF16)],
        compiler_params=pltpu.CompilerParams(vmem_limit_bytes=60 * 2 ** 20),
        cost_estimate=pl.CostEstimate(flops=flops, bytes_accessed=58 * 2 ** 20, transcendentals=0),
        name="second_pass",
    )(vc, pt_hot, slopes, *xds)


def token_grad_kernel(c_ref, uc_ref, dx_ref):
    width = uc_ref.shape[-1]
    dx_ref[...] = dot(c_ref[...], uc_ref[...].reshape(N_GRP * 256, width))


def token_grad(c_all, uc, first_set):
    width = uc.shape[-1]
    n_tok = c_all.shape[0] // N_SET
    flops = 2 * 2 * n_tok * N_GRP * 256 * width
    return pl.pallas_call(
        token_grad_kernel,
        grid=(2,),
        in_specs=[
            pl.BlockSpec((n_tok, N_GRP * 256), lambda i: (first_set + i, 0)),
            pl.BlockSpec((N_GRP, 1, 256, width), lambda i: (0, first_set + i, 0, 0)),
        ],
        out_specs=pl.BlockSpec((n_tok, width), lambda i: (i, 0)),
        out_shape=jax.ShapeDtypeStruct((2 * n_tok, width), F32),
        compiler_params=pltpu.CompilerParams(vmem_limit_bytes=60 * 2 ** 20),
        cost_estimate=pl.CostEstimate(flops=flops, bytes_accessed=16 * 2 ** 20, transcendentals=0),
        name="token_grad",
    )(c_all, uc)


def hot_tables(req_sets, core, zgrp):
    yx = jnp.arange(16)[:, None]
    z_of = jnp.where(zgrp == 0, jnp.array([0, 3]), jnp.array([1, 2]))[None, :]
    owners = ((z_of * 16 + yx) * 2 + core).reshape(N_OWN)
    req = jnp.stack([one[owners] for one in req_sets], axis=1)
    req = req.reshape(N_GRP, 2, 2, N_SET, REQ).transpose(0, 3, 1, 2, 4)
    row = (req + ROWS * jnp.arange(2)[:, None]).reshape(N_GRP, N_SET, 2, 2 * REQ)
    ids = jnp.arange(2 * ROWS)
    pt_hot = (row[..., None, :] == ids[:, None]).astype(BF16)
    p_hot = (row.transpose(0, 2, 1, 3).reshape(N_GRP, 2, N_SET * 128)[..., None] == ids).astype(BF16)
    return p_hot, pt_hot


def solution(mesh):
    tok_spec = P(('dp', 'ep'))
    table_spec = P('ep')
    plane = [[z * 32 + yx * 2 + c for yx in range(16)] for z in range(4) for c in range(2)]

    def swap(arr, mask):
        return lax.ppermute(arr, 'ep', [(i, i ^ mask) for i in range(N_EP)])

    def per_device(tokens, slot_ids, request_rows, gate_vals, grad_out, up_local, down_local):
        n_tok, width = tokens.shape
        n_sel = slot_ids.shape[1] * slot_ids.shape[2]
        index = lax.axis_index('ep')
        core, z_me = index % 2, index // 32
        zgrp = ((z_me + 1) // 2) % 2

        def table_rows(local):
            other = swap(local, ZTAB)
            both = jnp.where(z_me < 2, jnp.concatenate([local, other]), jnp.concatenate([other, local]))
            return lax.all_gather(both, 'ep', axis=0, tiled=True, axis_index_groups=plane)

        def grad_rows(part):
            mine = lax.psum_scatter(part, 'ep', scatter_dimension=0, tiled=True, axis_index_groups=plane)
            keep = lax.dynamic_slice_in_dim(mine, (z_me // 2) * ROWS, ROWS)
            give = lax.dynamic_slice_in_dim(mine, (1 - z_me // 2) * ROWS, ROWS)
            return (keep.astype(F32) + swap(give, ZTAB).astype(F32)).astype(BF16)

        def for_other_chip(remote_part):
            return remote_part[:n_tok] + swap(remote_part[n_tok:], CORE)

        def collect(local_part, from_z):
            from_core = swap(local_part[n_tok:], CORE)
            return (local_part[:n_tok] + from_core + from_z).astype(BF16)

        n_req = request_rows.shape[1] * request_rows.shape[2] // n_sel
        meta0 = jnp.concatenate([slot_ids.reshape(n_tok, n_sel).astype(F32), gate_vals.reshape(n_tok, n_sel), request_rows.reshape(n_req, n_sel).astype(F32)])
        xd0 = jnp.concatenate([tokens, grad_out])
        meta2 = swap(meta0, ZTOK)
        meta1 = swap(meta0, CORE)
        meta3 = swap(meta2, CORE)
        u_all = table_rows(up_local)
        v_all = table_rows(down_local)
        xd2 = swap(xd0, ZTOK)
        xd1 = swap(xd0, CORE)
        xd3 = swap(xd2, CORE)
        metas = (meta0, meta1, meta2, meta3)
        xds = (xd0, xd1, xd2, xd3)
        p_hot, pt_hot = hot_tables([m[2 * n_tok:].reshape(N_EP, REQ).astype(jnp.int32) for m in metas], core, zgrp)

        ctl = jnp.stack([core, zgrp]).astype(jnp.int32)
        gates = [gate_matrix(ctl, m, n_tok) for m in metas]
        uc, w_all, slopes, dv_part = first_pass(u_all, p_hot, pt_hot, gates, xds)
        vc, y_part = down_pass(v_all, p_hot, w_all)
        y_for_z, vc = lax.optimization_barrier((for_other_chip(y_part[2 * n_tok:]), vc))
        y_from_z = swap(y_for_z, ZTOK)
        c_all, du_part = second_pass(vc, pt_hot, slopes, xds)
        dx_rem = token_grad(c_all, uc, 2)
        dx_loc = token_grad(c_all, uc, 0)
        y = collect(y_part[:2 * n_tok], y_from_z)
        grad_down = grad_rows(dv_part)
        grad_up = grad_rows(du_part)
        dx = collect(dx_loc, swap(for_other_chip(dx_rem), ZTOK))
        return y, dx, grad_up, grad_down

    return jax.shard_map(per_device, mesh=mesh, in_specs=(tok_spec, tok_spec, tok_spec, tok_spec, tok_spec, table_spec, table_spec), out_specs=(tok_spec, tok_spec, tok_spec, tok_spec), check_vma=False)
```

```python
import functools
import math
import jax
import jax.numpy as jnp
from jax import lax
from jax.experimental import pallas as pl
from jax.experimental.pallas import tpu as pltpu
from jax.sharding import PartitionSpec as P


CORE, ZTOK, ZTAB = 1, 32, 96
N_EP, ROWS, REQ = 128, 128, 64
N_SET = 4
N_OWN = 32
N_GRP = N_OWN // 4
N_HI = N_OWN * REQ // 128
F32, BF16 = jnp.float32, jnp.bfloat16
NT = (((1,), (1,)), ((), ()))


def gelu_pair(pre_act):
    normal_cdf = 0.5 * (1.0 + lax.erf(pre_act * (2.0 ** -0.5)))
    normal_pdf = jnp.exp(-0.5 * pre_act * pre_act) * ((2.0 * math.pi) ** -0.5)
    return pre_act * normal_cdf, normal_cdf + pre_act * normal_pdf


def dot(a, b, dims=(((1,), (0,)), ((), ()))):
    return lax.dot_general(a, b, dims, preferred_element_type=F32)


def gate_kernel(ctl_ref, slot_ref, gate_ref, out_ref, hi_ref, lo_ref, g1_ref, g2_ref, g3_ref):
    n_tok = slot_ref.shape[0]
    slot = slot_ref[...].astype(jnp.int32)
    owner = slot >> 6
    z_of = owner >> 5
    here = ((owner & 1) == ctl_ref[0]) & ((((z_of + 1) >> 1) & 1) == ctl_ref[1])
    local = ((((owner >> 1) & 15) * 2 + (z_of >> 1)) << 6) + (slot & 63)
    hi_ref[...] = jnp.where(here, local >> 7, 255).astype(F32)
    lo_ref[...] = (local & 127).astype(F32)
    gate = gate_ref[...]
    g1 = gate.astype(BF16).astype(F32)
    g2 = (gate - g1).astype(BF16).astype(F32)
    g1_ref[...] = g1
    g2_ref[...] = g2
    g3_ref[...] = (gate - g1) - g2
    row_iota = lax.broadcasted_iota(jnp.int32, (16, 128), 0).astype(F32)
    iotas = [(row_iota + 16.0 * k).astype(BF16) for k in range(8)]
    out_flat = out_ref.reshape(n_tok * N_HI, 128)

    def spread(ref, t):
        return jnp.broadcast_to(ref[pl.ds(t, 1), :], (16, 128)).astype(BF16)

    def sides(t):
        hit = spread(hi_ref, t) == iotas[0]
        lhs = jnp.concatenate([jnp.where(hit, spread(ref, t), jnp.zeros((16, 128), BF16)) for ref in (g1_ref, g2_ref, g3_ref)], axis=0)
        lo_row = spread(lo_ref, t)
        rhs = jnp.concatenate([jnp.where(lo_row == one_iota, jnp.ones((16, 128), BF16), jnp.zeros((16, 128), BF16)) for one_iota in iotas], axis=0)
        return lhs, rhs

    def two_tokens(t):
        lhs_a, rhs_a = sides(t)
        lhs_b, rhs_b = sides(t + 1)
        empty = jnp.zeros_like(lhs_a)
        lhs = jnp.concatenate([jnp.concatenate([lhs_a, empty], axis=1), jnp.concatenate([empty, lhs_b], axis=1)], axis=0)
        res = dot(lhs, jnp.concatenate([rhs_a, rhs_b], axis=1), NT)
        return (res[32:48] + res[16:32]) + res[:16], (res[80:96] + res[64:80]) + res[48:64]

    def body(step, carry):
        for k in range(0, tok_step, 2):
            row_a, row_b = two_tokens(step * tok_step + k)
            base = (step * (tok_step // 8) + k // 8) * (8 * N_HI) + k % 8
            out_flat[pl.ds(base, N_HI, stride=8), :] = row_a
            out_flat[pl.ds(base + 1, N_HI, stride=8), :] = row_b
        return carry

    tok_step = min(64, n_tok)
    lax.fori_loop(0, n_tok // tok_step, body, 0)


def gate_matrix(ctl, meta, n_tok):
    tok_blk = min(256, n_tok)
    n_blk = n_tok // tok_blk
    return pl.pallas_call(
        gate_kernel,
        grid=(n_blk,),
        in_specs=[
            pl.BlockSpec(memory_space=pltpu.SMEM),
            pl.BlockSpec((tok_blk, 128), lambda i: (i, 0)),
            pl.BlockSpec((tok_blk, 128), lambda i: (i + n_blk, 0)),
        ],
        out_specs=pl.BlockSpec((tok_blk // 8, N_HI, 8, 128), lambda i: (i, 0, 0, 0)),
        out_shape=jax.ShapeDtypeStruct((n_tok // 8, N_HI, 8, 128), F32),
        scratch_shapes=[pltpu.VMEM((tok_blk, 128), F32)] * 5,
        compiler_params=pltpu.CompilerParams(vmem_limit_bytes=60 * 2 ** 20),
        cost_estimate=pl.CostEstimate(flops=n_tok * 12 * 2 ** 20, bytes_accessed=n_tok * 9216, transcendentals=0),
        name="gate_matrix",
    )(ctl, meta, meta)


def pick_rows(p_ref, table_ref, out_ref):
    for i in range(2):
        rows = dot(p_ref[0, i], table_ref[i * 256:(i + 1) * 256, :]).astype(BF16)
        for s in range(N_SET):
            out_ref[0, s, i * 128:(i + 1) * 128, :] = rows[s * 128:(s + 1) * 128]


def halves(n_tok):
    half = max(n_tok // 2, 16)
    return [slice(t, t + half) for t in range(0, n_tok, half)]


def first_kernel(n_tok, u_ref, p_ref, pt_ref, *refs):
    g_refs, x_refs, dy_refs = (refs[i * N_SET:(i + 1) * N_SET] for i in range(3))
    uc_ref, w_ref, s_ref, dv_ref, wrt, pre = refs[3 * N_SET:]
    tok_chunk = min(64, n_tok)

    def front(s):
        for part in halves(n_tok):
            pre[s, part, :] = dot(x_refs[s][part, :], uc_ref[0, s], NT)

    def back(s):
        for t0 in range(0, n_tok, tok_chunk):
            row0 = s * n_tok + t0
            for i in range(2):
                gate = g_refs[s][t0 // 8:(t0 + tok_chunk) // 8, i].reshape(tok_chunk, 128)
                act, slope = gelu_pair(pre[s, t0:t0 + tok_chunk, i * 128:(i + 1) * 128])
                used = gate > 0.0
                w_ref[row0:row0 + tok_chunk, i * 128:(i + 1) * 128] = jnp.where(used, gate * act, 0.0).astype(BF16)
                s_ref[row0:row0 + tok_chunk, i * 128:(i + 1) * 128] = jnp.where(used, gate * slope, 0.0)
        for i in range(2):
            wrt[i * 256:(i + 1) * 256, s * n_tok:(s + 1) * n_tok] = dot(pt_ref[0, s, i], w_ref[s * n_tok:(s + 1) * n_tok, i * 128:(i + 1) * 128], NT).astype(BF16)

    pick_rows(p_ref, u_ref, uc_ref)
    front(0)
    for s in range(1, N_SET):
        front(s)
        back(s - 1)
    back(N_SET - 1)
    dy_all = jnp.concatenate([ref[...] for ref in dy_refs], axis=0)
    dv_ref[...] = dot(wrt[...], dy_all).astype(BF16)


def whole(arr):
    return pl.BlockSpec(arr.shape, lambda g: (0,) * arr.ndim, pipeline_mode=pl.Buffered(1))


def first_pass(u_all, p_hot, pt_hot, gates, xs, dys):
    n_tok, width = xs[0].shape
    all_tok = N_SET * n_tok
    flops = 2 * N_GRP * N_SET * (256 * 256 * width + n_tok * width * 256 + n_tok * 128 * 512 + n_tok * 512 * width)
    return pl.pallas_call(
        functools.partial(first_kernel, n_tok),
        grid=(N_GRP,),
        in_specs=[
            pl.BlockSpec((512, width), lambda g: (g, 0)),
            pl.BlockSpec((1, 2, N_SET * 128, 256), lambda g: (g, 0, 0, 0)),
            pl.BlockSpec((1, N_SET, 2, 256, 128), lambda g: (g, 0, 0, 0, 0)),
        ] + [pl.BlockSpec((n_tok // 8, 2, 8, 128), lambda g: (0, g, 0, 0))] * N_SET + [whole(one) for one in (*xs, *dys)],
        out_specs=[
            pl.BlockSpec((1, N_SET, 256, width), lambda g: (g, 0, 0, 0)),
            pl.BlockSpec((all_tok, 256), lambda g: (0, g)),
            pl.BlockSpec((all_tok, 256), lambda g: (0, g)),
            pl.BlockSpec((512, width), lambda g: (g, 0)),
        ],
        out_shape=[
            jax.ShapeDtypeStruct((N_GRP, N_SET, 256, width), BF16),
            jax.ShapeDtypeStruct((all_tok, N_GRP * 256), BF16),
            jax.ShapeDtypeStruct((all_tok, N_GRP * 256), F32),
            jax.ShapeDtypeStruct((N_GRP * 512, width), BF16),
        ],
        scratch_shapes=[pltpu.VMEM((512, all_tok), BF16), pltpu.VMEM((N_SET, n_tok, 256), F32)],
        compiler_params=pltpu.CompilerParams(vmem_limit_bytes=60 * 2 ** 20),
        cost_estimate=pl.CostEstimate(flops=flops, bytes_accessed=76 * 2 ** 20, transcendentals=all_tok * N_GRP * 256),
        name="first_pass",
    )(u_all, p_hot, pt_hot, *gates, *xs, *dys)


def down_kernel(n_tok, v_ref, p_ref, w_ref, vc_ref, y_ref):
    @pl.when(pl.program_id(0) == 0)
    def _():
        y_ref[...] = jnp.zeros_like(y_ref)

    pick_rows(p_ref, v_ref, vc_ref)
    for s in range(N_SET):
        y_ref[s * n_tok:(s + 1) * n_tok, :] += dot(w_ref[s * n_tok:(s + 1) * n_tok, :], vc_ref[0, s])


def down_pass(v_all, p_hot, w_all):
    width = v_all.shape[1]
    all_tok = w_all.shape[0]
    n_tok = all_tok // N_SET
    flops = 2 * N_GRP * N_SET * (256 * 256 * width + n_tok * width * 256)
    return pl.pallas_call(
        functools.partial(down_kernel, n_tok),
        grid=(N_GRP,),
        in_specs=[
            pl.BlockSpec((512, width), lambda g: (g, 0)),
            pl.BlockSpec((1, 2, N_SET * 128, 256), lambda g: (g, 0, 0, 0)),
            pl.BlockSpec((all_tok, 256), lambda g: (0, g)),
        ],
        out_specs=[
            pl.BlockSpec((1, N_SET, 256, width), lambda g: (g, 0, 0, 0)),
            pl.BlockSpec((all_tok, width), lambda g: (0, 0)),
        ],
        out_shape=[
            jax.ShapeDtypeStruct((N_GRP, N_SET, 256, width), BF16),
            jax.ShapeDtypeStruct((all_tok, width), F32),
        ],
        compiler_params=pltpu.CompilerParams(vmem_limit_bytes=60 * 2 ** 20),
        cost_estimate=pl.CostEstimate(flops=flops, bytes_accessed=44 * 2 ** 20, transcendentals=0),
        name="down_pass",
    )(v_all, p_hot, w_all)


def second_kernel(n_tok, vc_ref, pt_ref, s_ref, *refs):
    x_refs, dy_refs = refs[:N_SET], refs[N_SET:2 * N_SET]
    c_ref, du_ref, crt = refs[2 * N_SET:]

    def front(s):
        for part in halves(n_tok):
            rows = slice(s * n_tok + part.start, s * n_tok + part.stop)
            back = dot(dy_refs[s][part, :], vc_ref[0, s], NT)
            slope = s_ref[rows, :]
            c_ref[rows, :] = jnp.where(slope == 0.0, 0.0, slope * back).astype(BF16)

    def back(s):
        rows = slice(s * n_tok, (s + 1) * n_tok)
        for i in range(2):
            crt[i * 256:(i + 1) * 256, rows] = dot(pt_ref[0, s, i], c_ref[rows, i * 128:(i + 1) * 128], NT).astype(BF16)

    front(0)
    for s in range(1, N_SET):
        front(s)
        back(s - 1)
    back(N_SET - 1)
    x_all = jnp.concatenate([ref[...] for ref in x_refs], axis=0)
    du_ref[...] = dot(crt[...], x_all).astype(BF16)


def second_pass(vc, pt_hot, slopes, xs, dys):
    n_tok, width = xs[0].shape
    all_tok = N_SET * n_tok
    flops = 2 * N_GRP * N_SET * (n_tok * width * 256 + n_tok * 128 * 512 + n_tok * 512 * width)
    return pl.pallas_call(
        functools.partial(second_kernel, n_tok),
        grid=(N_GRP,),
        in_specs=[
            pl.BlockSpec((1, N_SET, 256, width), lambda g: (g, 0, 0, 0)),
            pl.BlockSpec((1, N_SET, 2, 256, 128), lambda g: (g, 0, 0, 0, 0)),
            pl.BlockSpec((all_tok, 256), lambda g: (0, g)),
        ] + [whole(one) for one in (*xs, *dys)],
        out_specs=[
            pl.BlockSpec((all_tok, 256), lambda g: (0, g)),
            pl.BlockSpec((512, width), lambda g: (g, 0)),
        ],
        out_shape=[
            jax.ShapeDtypeStruct((all_tok, N_GRP * 256), BF16),
            jax.ShapeDtypeStruct((N_GRP * 512, width), BF16),
        ],
        scratch_shapes=[pltpu.VMEM((512, all_tok), BF16)],
        compiler_params=pltpu.CompilerParams(vmem_limit_bytes=60 * 2 ** 20),
        cost_estimate=pl.CostEstimate(flops=flops, bytes_accessed=58 * 2 ** 20, transcendentals=0),
        name="second_pass",
    )(vc, pt_hot, slopes, *xs, *dys)


def token_grad_kernel(c_ref, uc_ref, dx_ref):
    width = uc_ref.shape[-1]
    dx_ref[...] = dot(c_ref[...], uc_ref[...].reshape(N_GRP * 256, width))


def token_grad(c_all, uc, first_set):
    width = uc.shape[-1]
    n_tok = c_all.shape[0] // N_SET
    flops = 2 * 2 * n_tok * N_GRP * 256 * width
    return pl.pallas_call(
        token_grad_kernel,
        grid=(2,),
        in_specs=[
            pl.BlockSpec((n_tok, N_GRP * 256), lambda i: (first_set + i, 0)),
            pl.BlockSpec((N_GRP, 1, 256, width), lambda i: (0, first_set + i, 0, 0)),
        ],
        out_specs=pl.BlockSpec((n_tok, width), lambda i: (i, 0)),
        out_shape=jax.ShapeDtypeStruct((2 * n_tok, width), F32),
        compiler_params=pltpu.CompilerParams(vmem_limit_bytes=60 * 2 ** 20),
        cost_estimate=pl.CostEstimate(flops=flops, bytes_accessed=16 * 2 ** 20, transcendentals=0),
        name="token_grad",
    )(c_all, uc)


def ring_place():
    me = lax.axis_index('ep')
    core, x_me, y_me, z_me = me % 2, (me // 2) % 4, (me // 8) % 4, me // 32

    def device(z, y, x):
        return ((z * 4 + y) * 4 + x) * 2 + core

    return x_me, y_me, z_me, device


def meet(peers):
    barrier = pltpu.get_barrier_semaphore()
    for peer in peers:
        pl.semaphore_signal(barrier, inc=1, device_id={'ep': peer}, device_id_type=pl.DeviceIdType.MESH)
    pl.semaphore_wait(barrier, len(peers))


HALF_A, HALF_B, N_MSG = (2, 1), (3, 0), 19


def reduce_kernel(part_ref, out_ref, s1_prev, s1_next, s2_prev, s2_next, sum_next, sum_prev, mid, t1_prev, t1_next, t2_prev, t2_next, tsum_next, tsum_prev, keep, z_send, z_recv, send_sem, recv_sem):
    rows, width = out_ref.shape
    half = width // 2
    x_me, y_me, z_me, device = ring_place()
    z_peer = device(3 - z_me, y_me, x_me)
    upper = z_me // 2
    x_next, x_prev = device(z_me, y_me, (x_me + 1) % 4), device(z_me, y_me, (x_me + 3) % 4)
    y_next, y_prev = device(z_me, (y_me + 1) % 4, x_me), device(z_me, (y_me + 3) % 4, x_me)
    meet((x_next, x_prev, y_next, y_prev, z_peer))
    chunk = 32

    def add_up(n_rows, store, *loads):
        def step(i, carry):
            at = pl.ds(pl.multiple_of(i * chunk, chunk), chunk)
            total = loads[0](i, at)
            for load in loads[1:]:
                total = total + load(i, at)
            store(at, total)
            return carry

        lax.fori_loop(0, n_rows // chunk, step, 0)

    def from_buf(buf, *index):
        return lambda i, at: buf[(*index, at, slice(None))].astype(F32)

    def into_buf(buf, *index):
        def store(at, total):
            buf[(*index, at, slice(None))] = total.astype(buf.dtype)

        return store

    class Side:
        pass

    sides = []
    for k in range(2):
        one = Side()
        one.k = k
        first, second = (x_me, y_me) if k == 0 else (y_me, x_me)
        one.first, one.second = first, second
        one.next1, one.prev1 = (x_next, x_prev) if k == 0 else (y_next, y_prev)
        one.next2, one.prev2 = (y_next, y_prev) if k == 0 else (x_next, x_prev)
        sides.append(one)

    def start_of(one, shift1, shift2):
        first, second = (one.first + shift1) % 4, (one.second + shift2) % 4
        chip = second * 4 + first if one.k == 0 else first * 4 + second
        return chip * (2 * rows)

    def own(one, shift1, shift2):
        return part_ref.at[pl.ds(pl.multiple_of(start_of(one, shift1, shift2), 2 * rows), 2 * rows), pl.ds(one.k * half, half)]

    def load_own(one, shift1, shift2):
        start = start_of(one, shift1, shift2)
        return lambda i, at: part_ref[pl.ds(pl.multiple_of(start + i * chunk, chunk), chunk), one.k * half:(one.k + 1) * half].astype(F32)

    def message(one, number, src, dst, peer):
        return pltpu.make_async_remote_copy(
            src_ref=src, dst_ref=dst, send_sem=send_sem.at[one.k, number], recv_sem=recv_sem.at[one.k, number],
            device_id={'ep': peer}, device_id_type=pl.DeviceIdType.MESH)

    for one in sides:
        k = one.k
        one.s1n = [message(one, i, own(one, 2, HALF_A[i]), s1_prev.at[k, i], one.next1) for i in range(2)]
        one.s1p = [message(one, 2 + i, own(one, 2, HALF_B[i]), s1_next.at[k, i], one.prev1) for i in range(2)]
        one.inn = [message(one, 4 + i, own(one, 1, HALF_B[i]), s2_prev.at[k, HALF_B[i]], one.next1) for i in range(2)]
        one.inp = [message(one, 6 + i, own(one, 3, HALF_A[i]), s2_next.at[k, HALF_A[i]], one.prev1) for i in range(2)]
        one.dpn = [message(one, 8 + i, sum_next.at[k, i], s2_prev.at[k, HALF_A[i]], one.next1) for i in range(2)]
        one.dpp = [message(one, 10 + i, sum_prev.at[k, i], s2_next.at[k, HALF_B[i]], one.prev1) for i in range(2)]
        lower_rows, upper_rows = pl.ds(0, rows), pl.ds(rows, rows)
        one.t1n = message(one, 12, mid.at[k, 2, lower_rows], t1_prev.at[k], one.next2)
        one.t1p = message(one, 13, mid.at[k, 2, upper_rows], t1_next.at[k], one.prev2)
        one.tin = message(one, 14, mid.at[k, 1, upper_rows], t2_prev.at[k, 1], one.next2)
        one.tip = message(one, 15, mid.at[k, 3, lower_rows], t2_next.at[k, 0], one.prev2)
        one.tdn = message(one, 16, tsum_next.at[k], t2_prev.at[k, 0], one.next2)
        one.tdp = message(one, 17, tsum_prev.at[k], t2_next.at[k, 1], one.prev2)
        one.zz = message(one, 18, z_send.at[k], z_recv.at[k], z_peer)

    for i in range(2):
        for one in sides:
            one.s1n[i].start()
            one.s1p[i].start()
    for i in range(2):
        for one in sides:
            one.inn[i].start()
            one.inp[i].start()
    for i in range(2):
        for one in sides:
            one.s1n[i].wait_recv()
            add_up(2 * rows, into_buf(sum_next, one.k, i), load_own(one, 1, HALF_A[i]), from_buf(s1_prev, one.k, i))
            one.dpn[i].start()
            one.s1p[i].wait_recv()
            add_up(2 * rows, into_buf(sum_prev, one.k, i), load_own(one, 3, HALF_B[i]), from_buf(s1_next, one.k, i))
            one.dpp[i].start()
    for i, r in ((0, 2), (0, 3), (1, 1), (1, 0)):
        for one in sides:
            k = one.k
            if r in HALF_A:
                one.inp[i].wait_recv()
                one.dpn[i].wait_recv()
            else:
                one.inn[i].wait_recv()
                one.dpp[i].wait_recv()
            add_up(2 * rows, into_buf(mid, k, r), load_own(one, 0, r), from_buf(s2_prev, k, r), from_buf(s2_next, k, r))
            if r == 2:
                one.t1n.start()
                one.t1p.start()
            if r == 3:
                one.tip.start()
            if r == 1:
                one.tin.start()
    for one in sides:
        k = one.k
        one.t1n.wait_recv()
        add_up(rows, into_buf(tsum_next, k), from_buf(mid, k, 1), from_buf(t1_prev, k))
        one.tdn.start()
        one.t1p.wait_recv()
        add_up(rows, into_buf(tsum_prev, k), lambda i, at: mid[k, 3, pl.ds(pl.multiple_of(rows + i * chunk, chunk), chunk), :].astype(F32), from_buf(t1_next, k))
        one.tdp.start()
    for one in sides:
        k = one.k
        one.tin.wait_recv()
        one.tip.wait_recv()
        one.tdn.wait_recv()
        one.tdp.wait_recv()

        def last_sum(i, carry, k=k):
            at = pl.ds(pl.multiple_of(i * chunk, chunk), chunk)
            low = mid[k, 0, at, :].astype(F32) + t2_prev[k, 0, at, :].astype(F32) + t2_next[k, 0, at, :].astype(F32)
            high = mid[k, 0, pl.ds(pl.multiple_of(rows + i * chunk, chunk), chunk), :].astype(F32) + t2_prev[k, 1, at, :].astype(F32) + t2_next[k, 1, at, :].astype(F32)
            keep[k, at, :] = jnp.where(upper == 1, high, low)
            z_send[k, at, :] = jnp.where(upper == 1, low, high).astype(BF16)
            return carry

        lax.fori_loop(0, rows // chunk, last_sum, 0)
        one.zz.start()
    for one in sides:
        k = one.k
        one.zz.wait_recv()

        def store_out(at, total, k=k):
            out_ref[at, k * half:(k + 1) * half] = total.astype(BF16)

        add_up(rows, store_out, from_buf(keep, k), from_buf(z_recv, k))
    for one in sides:
        for msg in one.s1n + one.s1p + one.inn + one.inp + one.dpn + one.dpp + [one.t1n, one.t1p, one.tin, one.tip, one.tdn, one.tdp, one.zz]:
            msg.wait_send()


def reduce_rows(part):
    width = part.shape[1]
    rows = part.shape[0] // N_OWN
    half = width // 2
    big, small = (2 * rows, half), (rows, half)
    vmem = pl.BlockSpec(memory_space=pltpu.VMEM)
    return pl.pallas_call(
        reduce_kernel,
        in_specs=[vmem],
        out_specs=vmem,
        out_shape=jax.ShapeDtypeStruct((rows, width), BF16),
        scratch_shapes=[pltpu.VMEM(shape, BF16) for shape in ((2, 2, *big), (2, 2, *big), (2, 4, *big), (2, 4, *big), (2, 2, *big), (2, 2, *big), (2, 4, *big), (2, *small), (2, *small), (2, 2, *small), (2, 2, *small), (2, *small), (2, *small))]
        + [pltpu.VMEM((2, *small), F32), pltpu.VMEM((2, *small), BF16), pltpu.VMEM((2, *small), BF16), pltpu.SemaphoreType.DMA((2, N_MSG)), pltpu.SemaphoreType.DMA((2, N_MSG))],
        compiler_params=pltpu.CompilerParams(collective_id=0, has_side_effects=True, vmem_limit_bytes=48 * 2 ** 20),
        cost_estimate=pl.CostEstimate(flops=10 ** 9, bytes_accessed=part.size * 4, transcendentals=0),
        name="reduce_rows",
    )(part)


def hot_tables(req_sets, core, zgrp):
    yx = jnp.arange(16)[:, None]
    z_of = jnp.where(zgrp == 0, jnp.array([0, 3]), jnp.array([1, 2]))[None, :]
    owners = ((z_of * 16 + yx) * 2 + core).reshape(N_OWN)
    req = jnp.stack([one[owners] for one in req_sets], axis=1)
    req = req.reshape(N_GRP, 2, 2, N_SET, REQ).transpose(0, 3, 1, 2, 4)
    row = (req + ROWS * jnp.arange(2)[:, None]).reshape(N_GRP, N_SET, 2, 2 * REQ)
    ids = jnp.arange(2 * ROWS)
    pt_hot = (row[..., None, :] == ids[:, None]).astype(BF16)
    p_hot = (row.transpose(0, 2, 1, 3).reshape(N_GRP, 2, N_SET * 128)[..., None] == ids).astype(BF16)
    return p_hot, pt_hot


def solution(mesh):
    tok_spec = P(('dp', 'ep'))
    table_spec = P('ep')
    plane = [[z * 32 + yx * 2 + c for yx in range(16)] for z in range(4) for c in range(2)]

    def swap(arr, mask):
        return lax.ppermute(arr, 'ep', [(i, i ^ mask) for i in range(N_EP)])

    def device_part(tokens, slot_ids, request_rows, gate_vals, grad_out, up_local, down_local):
        n_tok, _ = tokens.shape
        n_sel = slot_ids.shape[1] * slot_ids.shape[2]
        index = lax.axis_index('ep')
        core, z_me = index % 2, index // 32
        zgrp = ((z_me + 1) // 2) % 2

        def table_rows(local):
            other = swap(local, ZTAB)
            both = jnp.where(z_me < 2, jnp.concatenate([local, other]), jnp.concatenate([other, local]))
            return lax.all_gather(both, 'ep', axis=0, tiled=True, axis_index_groups=plane)

        def grad_rows(part):
            mine = lax.psum_scatter(part, 'ep', scatter_dimension=0, tiled=True, axis_index_groups=plane)
            keep = lax.dynamic_slice_in_dim(mine, (z_me // 2) * ROWS, ROWS)
            give = lax.dynamic_slice_in_dim(mine, (1 - z_me // 2) * ROWS, ROWS)
            return (keep.astype(F32) + swap(give, ZTAB).astype(F32)).astype(BF16)

        def for_other_chip(remote_part):
            return remote_part[:n_tok] + swap(remote_part[n_tok:], CORE)

        def collect(local_part, from_z):
            from_core = swap(local_part[n_tok:], CORE)
            return (local_part[:n_tok] + from_core + from_z).astype(BF16)

        n_req = request_rows.shape[1] * request_rows.shape[2] // n_sel
        meta0 = jnp.concatenate([slot_ids.reshape(n_tok, n_sel).astype(F32), gate_vals.reshape(n_tok, n_sel), request_rows.reshape(n_req, n_sel).astype(F32)])
        meta2 = swap(meta0, ZTOK)
        meta1 = swap(meta0, CORE)
        meta3 = swap(meta2, CORE)
        x2 = swap(tokens, ZTOK)
        dy2 = swap(grad_out, ZTOK)
        u_all = table_rows(up_local)
        v_all = table_rows(down_local)
        xs = (tokens, swap(tokens, CORE), x2, swap(x2, CORE))
        dys = (grad_out, swap(grad_out, CORE), dy2, swap(dy2, CORE))
        metas = (meta0, meta1, meta2, meta3)
        p_hot, pt_hot = hot_tables([m[2 * n_tok:].reshape(N_EP, REQ).astype(jnp.int32) for m in metas], core, zgrp)

        ctl = jnp.stack([core, zgrp]).astype(jnp.int32)
        gates = []
        for meta in metas:
            gates.append(gate_matrix(ctl, meta, n_tok))
        uc, w_all, slopes, dv_part = first_pass(u_all, p_hot, pt_hot, gates, xs, dys)
        vc, y_part = down_pass(v_all, p_hot, w_all)
        y_for_z, vc = lax.optimization_barrier((for_other_chip(y_part[2 * n_tok:]), vc))
        y_from_z = swap(y_for_z, ZTOK)
        c_all, du_part = second_pass(vc, pt_hot, slopes, xs, dys)
        dx_rem = token_grad(c_all, uc, 2)
        dx_loc = token_grad(c_all, uc, 0)
        y = collect(y_part[:2 * n_tok], y_from_z)
        grad_down = grad_rows(dv_part)
        grad_up = reduce_rows(du_part)
        dx = collect(dx_loc, swap(for_other_chip(dx_rem), ZTOK))
        return y, dx, grad_up, grad_down

    return jax.shard_map(device_part, mesh=mesh, in_specs=(tok_spec, tok_spec, tok_spec, tok_spec, tok_spec, table_spec, table_spec), out_specs=(tok_spec, tok_spec, tok_spec, tok_spec), check_vma=False)
```

```python
import functools
import math
import jax
import jax.numpy as jnp
from jax import lax
from jax.experimental import pallas as pl
from jax.experimental.pallas import tpu as pltpu
from jax.sharding import PartitionSpec as P


CORE, ZTOK, ZTAB = 1, 32, 96
N_EP, ROWS, REQ = 128, 128, 64
N_SET = 4
N_OWN = 32
N_GRP = N_OWN // 4
N_HI = N_OWN * REQ // 128
F32, BF16 = jnp.float32, jnp.bfloat16
NT = (((1,), (1,)), ((), ()))


def gelu_pair(pre_act):
    normal_cdf = 0.5 * (1.0 + lax.erf(pre_act * (2.0 ** -0.5)))
    normal_pdf = jnp.exp(-0.5 * pre_act * pre_act) * ((2.0 * math.pi) ** -0.5)
    return pre_act * normal_cdf, normal_cdf + pre_act * normal_pdf


def dot(a, b, dims=(((1,), (0,)), ((), ()))):
    return lax.dot_general(a, b, dims, preferred_element_type=F32)


def gate_kernel(ctl_ref, slot_ref, gate_ref, out_ref, hi_ref, lo_ref, g1_ref, g2_ref, g3_ref):
    n_tok = slot_ref.shape[0]
    slot = slot_ref[...].astype(jnp.int32)
    owner = slot >> 6
    z_of = owner >> 5
    same_plane = z_of == ctl_ref[1]
    here = ((owner & 1) == ctl_ref[0]) & (same_plane | (z_of == 3 - ctl_ref[1]))
    local = ((((owner >> 1) & 15) * 2 + jnp.where(same_plane, 0, 1)) << 6) + (slot & 63)
    hi_ref[...] = jnp.where(here, local >> 7, 255).astype(F32)
    lo_ref[...] = (local & 127).astype(F32)
    gate = gate_ref[...]
    g1 = gate.astype(BF16).astype(F32)
    g2 = (gate - g1).astype(BF16).astype(F32)
    g1_ref[...] = g1
    g2_ref[...] = g2
    g3_ref[...] = (gate - g1) - g2
    row_iota = lax.broadcasted_iota(jnp.int32, (16, 128), 0).astype(F32)
    iotas = [(row_iota + 16.0 * k).astype(BF16) for k in range(8)]
    out_flat = out_ref.reshape(n_tok * N_HI, 128)

    def spread(ref, t):
        return jnp.broadcast_to(ref[pl.ds(t, 1), :], (16, 128)).astype(BF16)

    def sides(t):
        hit = spread(hi_ref, t) == iotas[0]
        lhs = jnp.concatenate([jnp.where(hit, spread(ref, t), jnp.zeros((16, 128), BF16)) for ref in (g1_ref, g2_ref, g3_ref)], axis=0)
        lo_row = spread(lo_ref, t)
        rhs = jnp.concatenate([jnp.where(lo_row == one_iota, jnp.ones((16, 128), BF16), jnp.zeros((16, 128), BF16)) for one_iota in iotas], axis=0)
        return lhs, rhs

    def two_tokens(t):
        lhs_a, rhs_a = sides(t)
        lhs_b, rhs_b = sides(t + 1)
        empty = jnp.zeros_like(lhs_a)
        lhs = jnp.concatenate([jnp.concatenate([lhs_a, empty], axis=1), jnp.concatenate([empty, lhs_b], axis=1)], axis=0)
        res = dot(lhs, jnp.concatenate([rhs_a, rhs_b], axis=1), NT)
        return (res[32:48] + res[16:32]) + res[:16], (res[80:96] + res[64:80]) + res[48:64]

    def body(step, carry):
        for k in range(0, tok_step, 2):
            row_a, row_b = two_tokens(step * tok_step + k)
            base = (step * (tok_step // 8) + k // 8) * (8 * N_HI) + k % 8
            out_flat[pl.ds(base, N_HI, stride=8), :] = row_a
            out_flat[pl.ds(base + 1, N_HI, stride=8), :] = row_b
        return carry

    tok_step = min(64, n_tok)
    lax.fori_loop(0, n_tok // tok_step, body, 0)


def gate_matrix(ctl, meta, n_tok):
    tok_blk = min(256, n_tok)
    n_blk = n_tok // tok_blk
    return pl.pallas_call(
        gate_kernel,
        grid=(n_blk,),
        in_specs=[
            pl.BlockSpec(memory_space=pltpu.SMEM),
            pl.BlockSpec((tok_blk, 128), lambda i: (i, 0)),
            pl.BlockSpec((tok_blk, 128), lambda i: (i + n_blk, 0)),
        ],
        out_specs=pl.BlockSpec((tok_blk // 8, N_HI, 8, 128), lambda i: (i, 0, 0, 0)),
        out_shape=jax.ShapeDtypeStruct((n_tok // 8, N_HI, 8, 128), F32),
        scratch_shapes=[pltpu.VMEM((tok_blk, 128), F32)] * 5,
        compiler_params=pltpu.CompilerParams(vmem_limit_bytes=60 * 2 ** 20),
        cost_estimate=pl.CostEstimate(flops=n_tok * 12 * 2 ** 20, bytes_accessed=n_tok * 9216, transcendentals=0),
        name="gate_matrix",
    )(ctl, meta, meta)


def pick_rows(p_ref, table_ref, out_ref):
    for i in range(2):
        rows = dot(p_ref[0, i], table_ref[i * 256:(i + 1) * 256, :]).astype(BF16)
        for s in range(N_SET):
            out_ref[0, s, i * 128:(i + 1) * 128, :] = rows[s * 128:(s + 1) * 128]


def halves(n_tok):
    half = max(n_tok // 2, 16)
    return [slice(t, t + half) for t in range(0, n_tok, half)]


def first_kernel(n_tok, u_ref, p_ref, pt_ref, *refs):
    g_refs, x_refs, dy_refs = (refs[i * N_SET:(i + 1) * N_SET] for i in range(3))
    uc_ref, w_ref, s_ref, dv_ref, wrt, pre = refs[3 * N_SET:]
    tok_chunk = min(64, n_tok)

    def front(s):
        for part in halves(n_tok):
            pre[s, part, :] = dot(x_refs[s][part, :], uc_ref[0, s], NT)

    def back(s):
        for t0 in range(0, n_tok, tok_chunk):
            row0 = s * n_tok + t0
            for i in range(2):
                gate = g_refs[s][t0 // 8:(t0 + tok_chunk) // 8, i].reshape(tok_chunk, 128)
                act, slope = gelu_pair(pre[s, t0:t0 + tok_chunk, i * 128:(i + 1) * 128])
                used = gate > 0.0
                w_ref[row0:row0 + tok_chunk, i * 128:(i + 1) * 128] = jnp.where(used, gate * act, 0.0).astype(BF16)
                s_ref[row0:row0 + tok_chunk, i * 128:(i + 1) * 128] = jnp.where(used, gate * slope, 0.0)
        for i in range(2):
            wrt[i * 256:(i + 1) * 256, s * n_tok:(s + 1) * n_tok] = dot(pt_ref[0, s, i], w_ref[s * n_tok:(s + 1) * n_tok, i * 128:(i + 1) * 128], NT).astype(BF16)

    pick_rows(p_ref, u_ref, uc_ref)
    front(0)
    for s in range(1, N_SET):
        front(s)
        back(s - 1)
    back(N_SET - 1)
    dy_all = jnp.concatenate([ref[...] for ref in dy_refs], axis=0)
    dv_ref[...] = dot(wrt[...], dy_all).astype(BF16)


def whole(arr):
    return pl.BlockSpec(arr.shape, lambda g: (0,) * arr.ndim, pipeline_mode=pl.Buffered(1))


def first_pass(u_all, p_hot, pt_hot, gates, xs, dys):
    n_tok, width = xs[0].shape
    all_tok = N_SET * n_tok
    flops = 2 * N_GRP * N_SET * (256 * 256 * width + n_tok * width * 256 + n_tok * 128 * 512 + n_tok * 512 * width)
    return pl.pallas_call(
        functools.partial(first_kernel, n_tok),
        grid=(N_GRP,),
        in_specs=[
            pl.BlockSpec((512, width), lambda g: (g, 0)),
            pl.BlockSpec((1, 2, N_SET * 128, 256), lambda g: (g, 0, 0, 0)),
            pl.BlockSpec((1, N_SET, 2, 256, 128), lambda g: (g, 0, 0, 0, 0)),
        ] + [pl.BlockSpec((n_tok // 8, 2, 8, 128), lambda g: (0, g, 0, 0))] * N_SET + [whole(one) for one in (*xs, *dys)],
        out_specs=[
            pl.BlockSpec((1, N_SET, 256, width), lambda g: (g, 0, 0, 0)),
            pl.BlockSpec((all_tok, 256), lambda g: (0, g)),
            pl.BlockSpec((all_tok, 256), lambda g: (0, g)),
            pl.BlockSpec((512, width), lambda g: (g, 0)),
        ],
        out_shape=[
            jax.ShapeDtypeStruct((N_GRP, N_SET, 256, width), BF16),
            jax.ShapeDtypeStruct((all_tok, N_GRP * 256), BF16),
            jax.ShapeDtypeStruct((all_tok, N_GRP * 256), F32),
            jax.ShapeDtypeStruct((N_GRP * 512, width), BF16),
        ],
        scratch_shapes=[pltpu.VMEM((512, all_tok), BF16), pltpu.VMEM((N_SET, n_tok, 256), F32)],
        compiler_params=pltpu.CompilerParams(vmem_limit_bytes=60 * 2 ** 20),
        cost_estimate=pl.CostEstimate(flops=flops, bytes_accessed=76 * 2 ** 20, transcendentals=all_tok * N_GRP * 256),
        name="first_pass",
    )(u_all, p_hot, pt_hot, *gates, *xs, *dys)


def down_kernel(n_tok, v_ref, p_ref, w_ref, vc_ref, *y_refs):
    @pl.when(pl.program_id(0) == 0)
    def _():
        for y_ref in y_refs:
            y_ref[...] = jnp.zeros_like(y_ref)

    pick_rows(p_ref, v_ref, vc_ref)
    for s in range(N_SET):
        y_refs[s][...] += dot(w_ref[s * n_tok:(s + 1) * n_tok, :], vc_ref[0, s])


def down_pass(v_all, p_hot, w_all):
    width = v_all.shape[1]
    all_tok = w_all.shape[0]
    n_tok = all_tok // N_SET
    flops = 2 * N_GRP * N_SET * (256 * 256 * width + n_tok * width * 256)
    return pl.pallas_call(
        functools.partial(down_kernel, n_tok),
        grid=(N_GRP,),
        in_specs=[
            pl.BlockSpec((512, width), lambda g: (g, 0)),
            pl.BlockSpec((1, 2, N_SET * 128, 256), lambda g: (g, 0, 0, 0)),
            pl.BlockSpec((all_tok, 256), lambda g: (0, g)),
        ],
        out_specs=[
            pl.BlockSpec((1, N_SET, 256, width), lambda g: (g, 0, 0, 0)),
        ] + [pl.BlockSpec((n_tok, width), lambda g: (0, 0))] * N_SET,
        out_shape=[
            jax.ShapeDtypeStruct((N_GRP, N_SET, 256, width), BF16),
        ] + [jax.ShapeDtypeStruct((n_tok, width), F32)] * N_SET,
        compiler_params=pltpu.CompilerParams(vmem_limit_bytes=60 * 2 ** 20),
        cost_estimate=pl.CostEstimate(flops=flops, bytes_accessed=44 * 2 ** 20, transcendentals=0),
        name="down_pass",
    )(v_all, p_hot, w_all)


def second_kernel(n_tok, vc_ref, pt_ref, s_ref, *refs):
    x_refs, dy_refs = refs[:N_SET], refs[N_SET:2 * N_SET]
    c_ref, du_ref, crt = refs[2 * N_SET:]

    def front(s):
        for part in halves(n_tok):
            rows = slice(s * n_tok + part.start, s * n_tok + part.stop)
            back = dot(dy_refs[s][part, :], vc_ref[0, s], NT)
            slope = s_ref[rows, :]
            c_ref[rows, :] = jnp.where(slope == 0.0, 0.0, slope * back).astype(BF16)

    def back(s):
        rows = slice(s * n_tok, (s + 1) * n_tok)
        for i in range(2):
            crt[i * 256:(i + 1) * 256, rows] = dot(pt_ref[0, s, i], c_ref[rows, i * 128:(i + 1) * 128], NT).astype(BF16)

    front(0)
    for s in range(1, N_SET):
        front(s)
        back(s - 1)
    back(N_SET - 1)
    x_all = jnp.concatenate([ref[...] for ref in x_refs], axis=0)
    du_ref[...] = dot(crt[...], x_all).astype(BF16)


def second_pass(vc, pt_hot, slopes, xs, dys):
    n_tok, width = xs[0].shape
    all_tok = N_SET * n_tok
    flops = 2 * N_GRP * N_SET * (n_tok * width * 256 + n_tok * 128 * 512 + n_tok * 512 * width)
    return pl.pallas_call(
        functools.partial(second_kernel, n_tok),
        grid=(N_GRP,),
        in_specs=[
            pl.BlockSpec((1, N_SET, 256, width), lambda g: (g, 0, 0, 0)),
            pl.BlockSpec((1, N_SET, 2, 256, 128), lambda g: (g, 0, 0, 0, 0)),
            pl.BlockSpec((all_tok, 256), lambda g: (0, g)),
        ] + [whole(one) for one in (*xs, *dys)],
        out_specs=[
            pl.BlockSpec((all_tok, 256), lambda g: (0, g)),
            pl.BlockSpec((512, width), lambda g: (g, 0)),
        ],
        out_shape=[
            jax.ShapeDtypeStruct((all_tok, N_GRP * 256), BF16),
            jax.ShapeDtypeStruct((N_GRP * 512, width), BF16),
        ],
        scratch_shapes=[pltpu.VMEM((512, all_tok), BF16)],
        compiler_params=pltpu.CompilerParams(vmem_limit_bytes=60 * 2 ** 20),
        cost_estimate=pl.CostEstimate(flops=flops, bytes_accessed=58 * 2 ** 20, transcendentals=0),
        name="second_pass",
    )(vc, pt_hot, slopes, *xs, *dys)


def ring_place():
    me = lax.axis_index('ep')
    core, x_me, y_me, z_me = me % 2, (me // 2) % 4, (me // 8) % 4, me // 32

    def device(z, y, x):
        return ((z * 4 + y) * 4 + x) * 2 + core

    return x_me, y_me, z_me, device


def meet(peers):
    barrier = pltpu.get_barrier_semaphore()
    for peer in peers:
        pl.semaphore_signal(barrier, inc=1, device_id={'ep': peer}, device_id_type=pl.DeviceIdType.MESH)
    pl.semaphore_wait(barrier, len(peers))


HALF_A, HALF_B, N_MSG, N_TILE = (2, 1), (3, 0), 19, 4


def tail_kernel(part_ref, c_ref, uc_ref, y0_ref, yc_ref, yz_ref, out_ref, dx_ref, y_ref,
                own_next, own_prev, own_mid, s1_prev, s1_next, s2_prev, s2_next, sum_next, sum_prev, mid,
                t1_prev, t1_next, t2_prev, t2_next, tsum_next, tsum_prev, keep, z_send, z_recv,
                c_buf, uc_buf, dx_part, core_recv, far_send, far_recv, y_in,
                send_sem, recv_sem, own_sem, load_sem, y_sem, core_send_sem, core_recv_sem, far_send_sem, far_recv_sem):
    rows, width = out_ref.shape
    half = width // 2
    n_tok = dx_ref.shape[0]
    tile = n_tok // N_TILE
    x_me, y_me, z_me, device = ring_place()
    me = lax.axis_index('ep')
    z_peer = device(3 - z_me, y_me, x_me)
    core_peer = me + 1 - 2 * (me % 2)
    far_peer = device(z_me + 1 - 2 * (z_me % 2), y_me, x_me)
    x_next, x_prev = device(z_me, y_me, (x_me + 1) % 4), device(z_me, y_me, (x_me + 3) % 4)
    y_next, y_prev = device(z_me, (y_me + 1) % 4, x_me), device(z_me, (y_me + 3) % 4, x_me)
    chunk = 32

    def load_set(s, slot):
        return (pltpu.make_async_copy(c_ref.at[pl.ds(s * n_tok, n_tok)], c_buf.at[slot], load_sem.at[s, 0]),
                pltpu.make_async_copy(uc_ref.at[:, s], uc_buf.at[slot], load_sem.at[s, 1]))

    loads = {s: load_set(s, s % 2) for s in range(N_SET)}
    for s in (3, 2):
        for copy in loads[s]:
            copy.start()
    meet((x_next, x_prev, y_next, y_prev, z_peer, core_peer, far_peer))

    def add_up(n_rows, store, *parts):
        def step(i, carry):
            at = pl.ds(pl.multiple_of(i * chunk, chunk), chunk)
            total = parts[0](i, at)
            for one_part in parts[1:]:
                total = total + one_part(i, at)
            store(at, total)
            return carry

        lax.fori_loop(0, n_rows // chunk, step, 0)

    def from_buf(buf, *index):
        return lambda i, at: buf[(*index, at, slice(None))].astype(F32)

    def into_buf(buf, *index):
        def store(at, total):
            buf[(*index, at, slice(None))] = total.astype(buf.dtype)

        return store

    class Side:
        pass

    sides = []
    for k in range(2):
        one = Side()
        one.k = k
        one.first, one.second = (x_me, y_me) if k == 0 else (y_me, x_me)
        one.next1, one.prev1 = (x_next, x_prev) if k == 0 else (y_next, y_prev)
        one.next2, one.prev2 = (y_next, y_prev) if k == 0 else (x_next, x_prev)
        sides.append(one)

    def own(one, shift1, shift2):
        first, second = (one.first + shift1) % 4, (one.second + shift2) % 4
        chip = second * 4 + first if one.k == 0 else first * 4 + second
        return part_ref.at[pl.ds(pl.multiple_of(chip * (2 * rows), 2 * rows), 2 * rows), pl.ds(one.k * half, half)]

    def remote(src, dst, sems, peer):
        return pltpu.make_async_remote_copy(src_ref=src, dst_ref=dst, send_sem=sems[0], recv_sem=sems[1],
                                            device_id={'ep': peer}, device_id_type=pl.DeviceIdType.MESH)

    def message(one, number, src, dst, peer):
        return remote(src, dst, (send_sem.at[one.k, number], recv_sem.at[one.k, number]), peer)

    lower_rows, upper_rows = pl.ds(0, rows), pl.ds(rows, rows)
    for one in sides:
        k = one.k
        one.s1n = [message(one, i, own(one, 2, HALF_A[i]), s1_prev.at[k, i], one.next1) for i in range(2)]
        one.s1p = [message(one, 2 + i, own(one, 2, HALF_B[i]), s1_next.at[k, i], one.prev1) for i in range(2)]
        one.inn = [message(one, 4 + i, own(one, 1, HALF_B[i]), s2_prev.at[k, HALF_B[i]], one.next1) for i in range(2)]
        one.inp = [message(one, 6 + i, own(one, 3, HALF_A[i]), s2_next.at[k, HALF_A[i]], one.prev1) for i in range(2)]
        one.dpn = [message(one, 8 + i, sum_next.at[k, i], s2_prev.at[k, HALF_A[i]], one.next1) for i in range(2)]
        one.dpp = [message(one, 10 + i, sum_prev.at[k, i], s2_next.at[k, HALF_B[i]], one.prev1) for i in range(2)]
        one.t1n = message(one, 12, mid.at[k, 2, lower_rows], t1_prev.at[k], one.next2)
        one.t1p = message(one, 13, mid.at[k, 2, upper_rows], t1_next.at[k], one.prev2)
        one.tin = message(one, 14, mid.at[k, 1, upper_rows], t2_prev.at[k, 1], one.next2)
        one.tip = message(one, 15, mid.at[k, 3, lower_rows], t2_next.at[k, 0], one.prev2)
        one.tdn = message(one, 16, tsum_next.at[k], t2_prev.at[k, 0], one.next2)
        one.tdp = message(one, 17, tsum_prev.at[k], t2_next.at[k, 1], one.prev2)
        one.zz = message(one, 18, z_send.at[k], z_recv.at[k], z_peer)
        one.stage = [pltpu.make_async_copy(own(one, 1, HALF_A[i]), own_next.at[k, i], own_sem.at[k, i]) for i in range(2)]
        one.stage += [pltpu.make_async_copy(own(one, 3, HALF_B[i]), own_prev.at[k, i], own_sem.at[k, 2 + i]) for i in range(2)]
        one.stage += [pltpu.make_async_copy(own(one, 0, r), own_mid.at[k, r], own_sem.at[k, 4 + r]) for r in range(4)]

    def core_msg(which, t):
        at = pl.ds(pl.multiple_of(t * tile, tile), tile)
        return remote(dx_part.at[3 - 2 * which, at], core_recv.at[which, at], (core_send_sem.at[which, t], core_recv_sem.at[which, t]), core_peer)

    def far_msg(t):
        at = pl.ds(pl.multiple_of(t * tile, tile), tile)
        return remote(far_send.at[at], far_recv.at[at], (far_send_sem.at[t], far_recv_sem.at[t]), far_peer)

    def tiles(body):
        lax.fori_loop(0, N_TILE, lambda t, carry: (body(t), carry)[1], 0)

    def dx_tile(s, t):
        at = pl.ds(pl.multiple_of(t * tile, tile), tile)
        dx_part[s, at, :] = dot(c_buf[s % 2, at, :], uc_buf[s % 2].reshape(N_GRP * 256, width))

    for i in range(2):
        for one in sides:
            one.s1n[i].start()
            one.s1p[i].start()
    for i in range(2):
        for one in sides:
            one.inn[i].start()
            one.inp[i].start()
    for one in sides:
        for copy in one.stage:
            copy.start()
    y_loads = [pltpu.make_async_copy(src, y_in.at[i], y_sem.at[i]) for i, src in enumerate((y0_ref, yc_ref, yz_ref))]
    for copy in y_loads:
        copy.start()

    for s in (3, 2):
        for copy in loads[s]:
            copy.wait()

    def far_tile(t):
        dx_tile(3, t)
        core_msg(0, t).start()
        dx_tile(2, t)

    tiles(far_tile)
    for s in (1, 0):
        for copy in loads[s]:
            copy.start()

    def far_sum(t):
        core_msg(0, t).wait_recv()

        def step(i, carry):
            at = pl.ds(pl.multiple_of(t * tile + i * 32, 32), 32)
            far_send[at, :] = dx_part[2, at, :] + core_recv[0, at, :]
            return carry

        lax.fori_loop(0, tile // 32, step, 0)
        far_msg(t).start()

    tiles(far_sum)

    for one in sides:
        for copy in one.stage:
            copy.wait()
    for i in range(2):
        for one in sides:
            k = one.k
            one.s1n[i].wait_recv()
            add_up(2 * rows, into_buf(sum_next, k, i), from_buf(own_next, k, i), from_buf(s1_prev, k, i))
            one.dpn[i].start()
            one.s1p[i].wait_recv()
            add_up(2 * rows, into_buf(sum_prev, k, i), from_buf(own_prev, k, i), from_buf(s1_next, k, i))
            one.dpp[i].start()

    for s in (1, 0):
        for copy in loads[s]:
            copy.wait()

    def near_tile(t):
        dx_tile(1, t)
        core_msg(1, t).start()
        dx_tile(0, t)

    tiles(near_tile)
    for copy in y_loads:
        copy.wait()

    def y_store(at, total):
        y_ref[at, :] = total.astype(BF16)

    add_up(n_tok, y_store, from_buf(y_in, 0), from_buf(y_in, 1), from_buf(y_in, 2))

    for i, r in ((0, 2), (0, 3), (1, 1), (1, 0)):
        for one in sides:
            k = one.k
            if r in HALF_A:
                one.inp[i].wait_recv()
                one.dpn[i].wait_recv()
            else:
                one.inn[i].wait_recv()
                one.dpp[i].wait_recv()
            add_up(2 * rows, into_buf(mid, k, r), from_buf(own_mid, k, r), from_buf(s2_prev, k, r), from_buf(s2_next, k, r))
            if r == 2:
                one.t1n.start()
                one.t1p.start()
            if r == 3:
                one.tip.start()
            if r == 1:
                one.tin.start()
    for one in sides:
        k = one.k
        one.t1n.wait_recv()
        add_up(rows, into_buf(tsum_next, k), from_buf(mid, k, 1), from_buf(t1_prev, k))
        one.tdn.start()
        one.t1p.wait_recv()
        add_up(rows, into_buf(tsum_prev, k), lambda i, at: mid[k, 3, pl.ds(pl.multiple_of(rows + i * chunk, chunk), chunk), :].astype(F32), from_buf(t1_next, k))
        one.tdp.start()
    for one in sides:
        k = one.k
        one.tin.wait_recv()
        one.tip.wait_recv()
        one.tdn.wait_recv()
        one.tdp.wait_recv()
        add_up(rows, into_buf(z_send, k), lambda i, at: mid[k, 0, pl.ds(pl.multiple_of(rows + i * chunk, chunk), chunk), :].astype(F32), from_buf(t2_prev, k, 1), from_buf(t2_next, k, 1))
        one.zz.start()
        add_up(rows, into_buf(keep, k), from_buf(mid, k, 0), from_buf(t2_prev, k, 0), from_buf(t2_next, k, 0))
    for one in sides:
        k = one.k
        one.zz.wait_recv()

        def store_out(at, total, k=k):
            out_ref[at, k * half:(k + 1) * half] = total.astype(BF16)

        add_up(rows, store_out, from_buf(keep, k), from_buf(z_recv, k))

    def last_tile(t):
        core_msg(1, t).wait_recv()
        far_msg(t).wait_recv()

        def step(i, carry):
            at = pl.ds(pl.multiple_of(t * tile + i * 32, 32), 32)
            dx_ref[at, :] = (dx_part[0, at, :] + core_recv[1, at, :] + far_recv[at, :]).astype(BF16)
            return carry

        lax.fori_loop(0, tile // 32, step, 0)

    tiles(last_tile)

    def sent(t):
        core_msg(0, t).wait_send()
        core_msg(1, t).wait_send()
        far_msg(t).wait_send()

    tiles(sent)
    for one in sides:
        for msg in one.s1n + one.s1p + one.inn + one.inp + one.dpn + one.dpp + [one.t1n, one.t1p, one.tin, one.tip, one.tdn, one.tdp, one.zz]:
            msg.wait_send()


def tail_pass(part, c_all, uc, y_own, y_core, y_far):
    width = part.shape[1]
    rows = part.shape[0] // N_OWN
    n_tok = y_own.shape[0]
    half = width // 2
    big, small, toks = (2 * rows, half), (rows, half), (n_tok, width)
    vmem = pl.BlockSpec(memory_space=pltpu.VMEM)
    hbm = pl.BlockSpec(memory_space=pl.ANY)
    dma = pltpu.SemaphoreType.DMA
    return pl.pallas_call(
        tail_kernel,
        in_specs=[hbm] * 6,
        out_specs=[vmem] * 3,
        out_shape=[jax.ShapeDtypeStruct((rows, width), BF16), jax.ShapeDtypeStruct(toks, BF16), jax.ShapeDtypeStruct(toks, BF16)],
        scratch_shapes=[pltpu.VMEM(shape, BF16) for shape in (
            (2, 2, *big), (2, 2, *big), (2, 4, *big), (2, 2, *big), (2, 2, *big), (2, 4, *big), (2, 4, *big), (2, 2, *big), (2, 2, *big), (2, 4, *big),
            (2, *small), (2, *small), (2, 2, *small), (2, 2, *small), (2, *small), (2, *small))]
        + [pltpu.VMEM((2, *small), F32), pltpu.VMEM((2, *small), BF16), pltpu.VMEM((2, *small), BF16),
           pltpu.VMEM((2, n_tok, N_GRP * 256), BF16), pltpu.VMEM((2, N_GRP, 256, width), BF16),
           pltpu.VMEM((N_SET, *toks), F32), pltpu.VMEM((2, *toks), F32), pltpu.VMEM(toks, F32), pltpu.VMEM(toks, F32), pltpu.VMEM((3, *toks), F32),
           dma((2, N_MSG)), dma((2, N_MSG)), dma((2, 8)), dma((N_SET, 2)), dma((3,)),
           dma((2, N_TILE)), dma((2, N_TILE)), dma((N_TILE,)), dma((N_TILE,))],
        compiler_params=pltpu.CompilerParams(collective_id=0, has_side_effects=True, vmem_limit_bytes=60 * 2 ** 20),
        cost_estimate=pl.CostEstimate(flops=2 * N_SET * n_tok * N_GRP * 256 * width, bytes_accessed=40 * 2 ** 20, transcendentals=0),
        name="tail_pass",
    )(part, c_all, uc, y_own, y_core, y_far)


def hot_tables(req_sets, core, z_me):
    yx = jnp.arange(16)[:, None]
    z_of = jnp.stack([z_me, 3 - z_me])[None, :]
    owners = ((z_of * 16 + yx) * 2 + core).reshape(N_OWN)
    req = jnp.stack([one[owners] for one in req_sets], axis=1)
    req = req.reshape(N_GRP, 2, 2, N_SET, REQ).transpose(0, 3, 1, 2, 4)
    row = (req + ROWS * jnp.arange(2)[:, None]).reshape(N_GRP, N_SET, 2, 2 * REQ)
    ids = jnp.arange(2 * ROWS)
    pt_hot = (row[..., None, :] == ids[:, None]).astype(BF16)
    p_hot = (row.transpose(0, 2, 1, 3).reshape(N_GRP, 2, N_SET * 128)[..., None] == ids).astype(BF16)
    return p_hot, pt_hot


def solution(mesh):
    tok_spec = P(('dp', 'ep'))
    table_spec = P('ep')
    plane = [[z * 32 + yx * 2 + c for yx in range(16)] for z in range(4) for c in range(2)]

    def swap(arr, mask):
        return lax.ppermute(arr, 'ep', [(i, i ^ mask) for i in range(N_EP)])

    def device_part(tokens, slot_ids, request_rows, gate_vals, grad_out, up_local, down_local):
        n_tok, _ = tokens.shape
        n_sel = slot_ids.shape[1] * slot_ids.shape[2]
        index = lax.axis_index('ep')
        core, z_me = index % 2, index // 32

        def table_rows(local):
            both = jnp.concatenate([local, swap(local, ZTAB)])
            return lax.all_gather(both, 'ep', axis=0, tiled=True, axis_index_groups=plane)

        def grad_rows(part, after):
            mine = lax.psum_scatter(part, 'ep', scatter_dimension=0, tiled=True, axis_index_groups=plane)
            mine, _ = lax.optimization_barrier((mine, after))
            return (mine[:ROWS].astype(F32) + swap(mine[ROWS:], ZTAB).astype(F32)).astype(BF16)

        n_req = request_rows.shape[1] * request_rows.shape[2] // n_sel
        meta0 = jnp.concatenate([slot_ids.reshape(n_tok, n_sel).astype(F32), gate_vals.reshape(n_tok, n_sel), request_rows.reshape(n_req, n_sel).astype(F32)])
        meta2 = swap(meta0, ZTOK)
        meta1 = swap(meta0, CORE)
        meta3 = swap(meta2, CORE)
        x2 = swap(tokens, ZTOK)
        dy2 = swap(grad_out, ZTOK)
        u_all = table_rows(up_local)
        v_all = table_rows(down_local)
        xs = (tokens, swap(tokens, CORE), x2, swap(x2, CORE))
        dys = (grad_out, swap(grad_out, CORE), dy2, swap(dy2, CORE))
        metas = (meta0, meta1, meta2, meta3)
        p_hot, pt_hot = hot_tables([m[2 * n_tok:].reshape(N_EP, REQ).astype(jnp.int32) for m in metas], core, z_me)

        ctl = jnp.stack([core, z_me]).astype(jnp.int32)
        gates = []
        for meta in metas:
            gates.append(gate_matrix(ctl, meta, n_tok))
        uc, w_all, slopes, dv_part = first_pass(u_all, p_hot, pt_hot, gates, xs, dys)
        vc, *y_parts = down_pass(v_all, p_hot, w_all)
        y_for_far, vc = lax.optimization_barrier((y_parts[2] + swap(y_parts[3], CORE), vc))
        y_far = swap(y_for_far, ZTOK)
        y_core = swap(y_parts[1], CORE)
        c_all, du_part = second_pass(vc, pt_hot, slopes, xs, dys)
        grad_up, dx, y = tail_pass(du_part, c_all, uc, y_parts[0], y_core, y_far)
        grad_down = grad_rows(dv_part, grad_up)
        return y, dx, grad_up, grad_down

    return jax.shard_map(device_part, mesh=mesh, in_specs=(tok_spec, tok_spec, tok_spec, tok_spec, tok_spec, table_spec, table_spec), out_specs=(tok_spec, tok_spec, tok_spec, tok_spec), check_vma=False)
```

```python
import functools
import math
import jax
import jax.numpy as jnp
from jax import lax
from jax.experimental import pallas as pl
from jax.experimental.pallas import tpu as pltpu
from jax.sharding import PartitionSpec as P


CORE, ZTOK, ZTAB = 1, 32, 96
N_EP = ROWS = LANES = 128
REQ, SUB, TILE, RING = 64, 16, 8, 4
OWN, NEXT, OPP, PREV = range(RING)
HERE, THERE = UP, DOWN = PAIR = range(2)
N_SET, N_OWN = 4, 32
SETS = range(N_SET)
SET_ME, SET_CORE, SET_FAR, SET_FAR_CORE = SETS
CHIPS = N_OWN // 2
N_GRP = CHIPS // 2
N_HI = N_OWN * REQ // LANES
WIDE = 2 * LANES
G_ROWS = 2 * WIDE
MIB = 2 ** 20
ALL_VMEM = 60 * MIB
F32, BF16 = jnp.float32, jnp.bfloat16
NN, NT = ((((1,), (side,)), ((), ())) for side in PAIR)


def span(i, size):
    return slice(i * size, (i + 1) * size)


def aligned(start, size):
    return pl.ds(pl.multiple_of(start, size), size)


def steps(count, body):
    lax.fori_loop(0, count, lambda i, carry: (body(i), carry)[1], 0)


def start_all(copies):
    for copy in copies:
        copy.start()


def wait_all(copies):
    for copy in copies:
        copy.wait()


def gelu_pair(pre_act):
    normal_cdf = 0.5 * (1.0 + lax.erf(pre_act * (2.0 ** -0.5)))
    normal_pdf = jnp.exp(-0.5 * pre_act * pre_act) * ((2.0 * math.pi) ** -0.5)
    return pre_act * normal_cdf, normal_cdf + pre_act * normal_pdf


def dot(a, b, dims=NN):
    return lax.dot_general(a, b, dims, preferred_element_type=F32)


class Side:
    pass


class Place:
    def __init__(self):
        me = lax.axis_index('ep')
        self.core, x, y, z = me % 2, (me // 2) % RING, (me // TILE) % RING, me // N_OWN
        self.z = z

        def device(z_to, y_to, x_to):
            return ((z_to * RING + y_to) * RING + x_to) * 2 + self.core

        self.plane_peer = device(3 - z, y, x)
        self.core_peer = me + 1 - 2 * self.core
        self.far_peer = device(z + 1 - 2 * (z % 2), y, x)
        along_x = [device(z, y, (x + step) % RING) for step in (NEXT, PREV)]
        along_y = [device(z, (y + step) % RING, x) for step in (NEXT, PREV)]
        self.peers = (*along_x, *along_y, self.plane_peer, self.core_peer, self.far_peer)
        self.chip = y * RING + x
        self.sides = []
        for k, (first, second, axes) in enumerate(((x, y, (along_x, along_y)), (y, x, (along_y, along_x)))):
            one = Side()
            one.k, one.first, one.second = k, first, second
            one.axis1, one.axis2 = axes
            self.sides.append(one)

    def meet(self):
        barrier = pltpu.get_barrier_semaphore()
        for peer in self.peers:
            pl.semaphore_signal(barrier, inc=1, device_id={'ep': peer}, device_id_type=pl.DeviceIdType.MESH)
        pl.semaphore_wait(barrier, len(self.peers))


def chip_at(one, shift1, shift2):
    first, second = (one.first + shift1) % RING, (one.second + shift2) % RING
    return first * RING + second if one.k else second * RING + first


def remote(src, dst, sems, index, peer):
    return pltpu.make_async_remote_copy(src_ref=src, dst_ref=dst, send_sem=sems[UP].at[index], recv_sem=sems[DOWN].at[index],
                                        device_id={'ep': peer}, device_id_type=pl.DeviceIdType.MESH)


NEAR1, FAR1, NEAR2, FAR2, N_PIECE = 0, 4, 6, 22, 30
TOK_STEP = 64


def head_kernel(x_ref, dy_ref, meta_ref, u_ref, v_ref,
                u_all, v_far, x1, x2, x3, dy1, dy2, dy3, g0, g1, g2, g3, p_hot, pt_hot,
                u_own, meta_v, gates_v, hi_ref, lo_ref, a1_ref, a2_ref, a3_ref, row_v, p_v, pt_v,
                u_send, u_recv, meta_send, meta_recv, tok_send, tok_recv, tab_send, tab_recv, u_sem, meta_sem, gate_sem, p_sem, pt_sem):
    n_tok, width = x_ref.shape
    rows = u_ref.shape[0]
    half = width // 2
    n_chunk = n_tok // TOK_STEP
    at = Place()
    sides = at.sides

    load_u = pltpu.make_async_copy(u_ref, u_own, u_sem)
    load_meta = pltpu.make_async_copy(meta_ref, meta_v.at[SET_ME], meta_sem)
    start_all((load_u, load_meta))
    at.meet()

    chip_row = at.chip * (2 * rows)
    meta_sems, tok_sems, tab_sems = (meta_send, meta_recv), (tok_send, tok_recv), (tab_send, tab_recv)
    meta_core = remote(meta_ref, meta_v.at[SET_CORE], meta_sems, SET_ME, at.core_peer)
    meta_far = remote(meta_ref, meta_v.at[SET_FAR], meta_sems, SET_CORE, at.far_peer)
    meta_pass = remote(meta_v.at[SET_FAR], meta_v.at[SET_FAR_CORE], meta_sems, SET_FAR, at.core_peer)
    tok_far = [remote(src, dst, tok_sems, (SET_ME, i), at.far_peer) for i, (src, dst) in enumerate(((x_ref, x2), (dy_ref, dy2)))]
    tok_core = [remote(src, dst, tok_sems, (SET_CORE, i), at.core_peer) for i, (src, dst) in enumerate(((x_ref, x1), (dy_ref, dy1)))]
    tok_pass = [remote(src, dst, tok_sems, (SET_FAR, i), at.core_peer) for i, (src, dst) in enumerate(((x2, x3), (dy2, dy3)))]
    swap_u = remote(u_ref, u_all.at[aligned(chip_row + rows, rows)], tab_sems, UP, at.plane_peer)
    swap_v = remote(v_ref, v_far, tab_sems, DOWN, at.plane_peer)

    def piece(one, shift1, shift2, w):
        return u_all.at[aligned(chip_at(one, shift1, shift2) * (2 * rows) + w * rows, rows), pl.ds(one.k * half, half)]

    def copy_of(one, number, src, dst, peer):
        return remote(src, dst, (u_send, u_recv), (one.k, number), peer)

    def send(one, number, shift1, shift2, w, peer):
        place = piece(one, shift1, shift2, w)
        mine = (shift1, shift2, w) == (OWN, OWN, HERE)
        copy_of(one, number, u_own.at[:, pl.ds(one.k * half, half)] if mine else place, place, peer).start()

    def landed(one, number, shift1, shift2, w):
        place = piece(one, shift1, shift2, w)
        copy_of(one, number, place, place, one.axis1[UP]).wait_recv()

    def spread_first(one, w):
        for d in PAIR:
            send(one, NEAR1 + d * 2 + w, OWN, OWN, w, one.axis1[d])

    def spread_second(one, r, w):
        for d in PAIR:
            send(one, NEAR2 + d * TILE + r * 2 + w, r, OWN, w, one.axis2[d])

    def pass_second(one, r, w):
        back = NEXT if w else PREV
        landed(one, NEAR2 + w * TILE + r * 2 + w, r, back, w)
        send(one, FAR2 + r * 2 + w, r, back, w, one.axis2[w])

    def near_pieces(w):
        for one in sides:
            landed(one, NEAR1 + w, PREV, OWN, w)
            if w == HERE:
                send(one, FAR1 + w, PREV, OWN, w, one.axis1[UP])
            spread_second(one, PREV, w)
            landed(one, NEAR1 + 2 + w, NEXT, OWN, w)
            if w == THERE:
                send(one, FAR1 + w, NEXT, OWN, w, one.axis1[DOWN])
            spread_second(one, NEXT, w)

    def partner_plane():
        swap_u.wait_recv()
        for one in sides:
            spread_first(one, THERE)
            spread_second(one, OWN, THERE)

    def opposite_pieces(w):
        for one in sides:
            landed(one, FAR1 + w, OPP, OWN, w)
            spread_second(one, OPP, w)

    def pass_on(w, *which):
        for r in which:
            for one in sides:
                pass_second(one, r, w)

    def meta_arrives():
        meta_far.wait_recv()
        meta_pass.start()

    events = (
        (4, lambda: near_pieces(HERE)),
        (7, partner_plane),
        (8, meta_core.wait_recv),
        (9, lambda: opposite_pieces(HERE)),
        (13, meta_arrives),
        (14, lambda: pass_on(HERE, OWN)),
        (17, lambda: near_pieces(THERE)),
        (20, lambda: pass_on(HERE, PREV, NEXT)),
        (22, lambda: opposite_pieces(THERE)),
        (24, meta_pass.wait_recv),
        (25, lambda: pass_on(HERE, OPP)),
        (27, lambda: pass_on(THERE, OWN)),
        (29, lambda: pass_on(THERE, PREV, NEXT)),
    )

    start_all((meta_far, swap_u, swap_v, meta_core))
    load_u.wait()
    for one in sides:
        spread_first(one, HERE)
        spread_second(one, OWN, HERE)
    store_u = pltpu.make_async_copy(u_own, u_all.at[aligned(chip_row, rows)], u_sem)
    start_all((store_u, *tok_far, *tok_core))
    load_meta.wait()

    packed = (SUB, LANES)
    row_iota = lax.broadcasted_iota(jnp.int32, packed, 0).astype(F32)
    iotas = [(row_iota + float(SUB) * k).astype(BF16) for k in range(SUB)]
    zero, unit = jnp.zeros(packed, BF16), jnp.ones(packed, BF16)

    def set_up(s):
        slot = meta_v[s, :n_tok, :].astype(jnp.int32)
        owner = slot >> 6
        z_of = owner >> 5
        same_plane = z_of == at.z
        here = ((owner & 1) == at.core) & (same_plane | (z_of == 3 - at.z))
        local = ((((owner >> 1) & 15) * 2 + jnp.where(same_plane, HERE, THERE)) << 6) + (slot & 63)
        hi_ref[...] = jnp.where(here, local >> 7, 255).astype(F32)
        lo_ref[...] = (local & 127).astype(F32)
        gate = meta_v[s, span(1, n_tok), :]
        first = gate.astype(BF16).astype(F32)
        second = (gate - first).astype(BF16).astype(F32)
        a1_ref[...] = first
        a2_ref[...] = second
        a3_ref[...] = (gate - first) - second

    def spread(row):
        return jnp.broadcast_to(row, packed).astype(BF16)

    def one_hot(row, count):
        return jnp.concatenate([jnp.where(row == one_iota, unit, zero) for one_iota in iotas[:count]], axis=0)

    def one_token(t):
        row = pl.ds(t, 1)
        hit = spread(hi_ref[row, :]) == iotas[0]
        lhs = jnp.concatenate([jnp.where(hit, spread(ref[row, :]), zero) for ref in (a1_ref, a2_ref, a3_ref)], axis=0)
        return lhs, one_hot(spread(lo_ref[row, :]), TILE)

    def two_tokens(t):
        lhs_a, rhs_a = one_token(t)
        lhs_b, rhs_b = one_token(t + 1)
        empty = jnp.zeros_like(lhs_a)
        lhs = jnp.concatenate([jnp.concatenate(pair, axis=1) for pair in ((lhs_a, empty), (empty, lhs_b))], axis=0)
        res = dot(lhs, jnp.concatenate([rhs_a, rhs_b], axis=1), NT)
        low_a, mid_a, top_a, low_b, mid_b, top_b = (res[span(k, SUB)] for k in range(6))
        return (top_a + mid_a) + low_a, (top_b + mid_b) + low_b

    def gate_step(i):
        for when, event in events:
            pl.when(i == when * n_chunk // TILE)(event)
        s, j = i // n_chunk, i % n_chunk
        pl.when(j == 0)(lambda: set_up(s))
        for k in range(0, TOK_STEP, 2):
            base = (i * (TOK_STEP // TILE) + k // TILE) * (TILE * N_HI) + k % TILE
            for which, row in enumerate(two_tokens(j * TOK_STEP + k)):
                gates_v[pl.ds(base + which, N_HI, stride=TILE), :] = row

    steps(N_SET * n_chunk, gate_step)
    gate_out = [pltpu.make_async_copy(gates_v.at[pl.ds(s * n_tok * N_HI, n_tok * N_HI)], ref, gate_sem.at[s]) for s, ref in enumerate((g0, g1, g2, g3))]
    start_all(gate_out)
    pass_on(THERE, OPP)

    for s in SETS:
        asked = [meta_v[s, pl.ds(2 * n_tok + z_of * CHIPS, CHIPS), :] for z_of in (at.z, 3 - at.z)]
        turned = [jnp.concatenate([one_req[:, REQ:], one_req[:, :REQ]], axis=1) for one_req in asked]
        low_core = at.core == 0
        lane = lax.broadcasted_iota(jnp.int32, (CHIPS, LANES), 1)
        row_v[s] = jnp.where(lane < REQ, jnp.where(low_core, asked[HERE], turned[HERE]), jnp.where(low_core, turned[THERE], asked[THERE]) + float(ROWS))

    def hot_step(chip):
        for s in SETS:
            hot = one_hot(spread(row_v[s, pl.ds(chip, 1), :]), SUB)
            pt_v[chip, s] = hot
            p_v[chip, span(s, LANES), :] = hot.astype(F32).T.astype(BF16)

    steps(CHIPS, hot_step)
    hot_out = [pltpu.make_async_copy(p_v, p_hot, p_sem), pltpu.make_async_copy(pt_v, pt_hot, pt_sem)]
    start_all(hot_out)

    tok_far[UP].wait_recv()
    tok_pass[UP].start()
    for one in sides:
        for r in range(RING):
            landed(one, NEAR2 + TILE + r * 2, r, NEXT, HERE)
            landed(one, NEAR2 + r * 2 + 1, r, PREV, THERE)
    for one in sides:
        for r in range(RING):
            for w in PAIR:
                landed(one, FAR2 + r * 2 + w, r, OPP, w)
    swap_v.wait_recv()
    tok_far[DOWN].wait_recv()
    tok_pass[DOWN].start()
    for copy in tok_core + tok_pass:
        copy.wait_recv()
    wait_all(gate_out + hot_out + [store_u])
    for one in sides:
        for number in range(N_PIECE):
            place = piece(one, OWN, OWN, HERE)
            copy_of(one, number, place, place, one.axis1[UP]).wait_send()
    for copy in tok_far + tok_core + tok_pass + [meta_core, meta_far, meta_pass, swap_u, swap_v]:
        copy.wait_send()


def vmem(dtype, *shapes):
    return [pltpu.VMEM(shape, dtype) for shape in shapes]


def dma_sems(*shapes):
    return [pltpu.SemaphoreType.DMA(shape) for shape in shapes]


def arrays(dtype, *shapes):
    return [jax.ShapeDtypeStruct(shape, dtype) for shape in shapes]


def kernel(body, out_shape, scratch, flops, mib, grid=(), comm=None, **specs):
    extra = {} if comm is None else dict(collective_id=comm, has_side_effects=True)
    return pl.pallas_call(
        body, grid=grid, out_shape=out_shape, scratch_shapes=scratch,
        compiler_params=pltpu.CompilerParams(vmem_limit_bytes=ALL_VMEM, **extra),
        cost_estimate=pl.CostEstimate(flops=flops, bytes_accessed=mib * MIB, transcendentals=0), **specs)


ANY, IN_VMEM = pl.BlockSpec(memory_space=pl.ANY), pl.BlockSpec(memory_space=pltpu.VMEM)


def head_pass(x, dy, meta, u_local, v_local):
    n_tok, width = x.shape
    rows = u_local.shape[0]
    gate, p_shape, pt_shape = (n_tok * N_HI, LANES), (CHIPS, N_SET * LANES, WIDE), (CHIPS, N_SET, WIDE, LANES)
    outs = arrays(BF16, (N_OWN * rows, width), u_local.shape, *[x.shape] * 6) + arrays(F32, *[gate] * N_SET) + arrays(BF16, p_shape, pt_shape)
    pieces, three, six, two = (2, N_PIECE), (3,), (3, 2), (2,)
    scratch = vmem(BF16, u_local.shape) + vmem(F32, (N_SET, *meta.shape), (N_SET * n_tok * N_HI, LANES), *[(n_tok, LANES)] * 5, (N_SET, CHIPS, LANES))
    scratch += vmem(BF16, p_shape, pt_shape) + dma_sems(pieces, pieces, three, three, six, six, two, two, (), (), (N_SET,), (), ())
    u_all, v_far, x1, x2, x3, dy1, dy2, dy3, *gates, p_hot, pt_hot = kernel(
        head_kernel, outs, scratch, N_SET * n_tok * 12 * MIB, 60, comm=1,
        in_specs=[ANY] * 5, out_specs=[ANY] * len(outs))(x, dy, meta, u_local, v_local)
    gates = [one.reshape(n_tok // TILE, N_HI, TILE, LANES) for one in gates]
    return u_all, v_far, (x, x1, x2, x3), (dy, dy1, dy2, dy3), gates, p_hot.reshape(N_GRP, 2, *p_shape[1:]), pt_hot.reshape(N_GRP, 2, *pt_shape[1:])


def block(shape, axis=0):
    return pl.BlockSpec(shape, lambda g: tuple(g if k == axis else 0 for k in range(len(shape))))


def whole(arr):
    return pl.BlockSpec(arr.shape, lambda g: (0,) * arr.ndim, pipeline_mode=pl.Buffered(1))


P_BLOCK, PT_BLOCK = block((1, 2, N_SET * LANES, WIDE)), block((1, 2, N_SET, WIDE, LANES))


def pick_rows(p_ref, tables, out_ref):
    for i in PAIR:
        rows = dot(p_ref[0, i], tables[i]).astype(BF16)
        for s in SETS:
            out_ref[0, s, span(i, LANES), :] = rows[span(s, LANES)]


def halves(n_tok):
    half = max(n_tok // 2, SUB)
    return [slice(t, t + half) for t in range(0, n_tok, half)]


def staggered(front, back):
    for s in SETS:
        front(s)
        if s:
            back(s - 1)
    back(SET_FAR_CORE)


def spread_slots(pt_ref, values_ref, out, s, n_tok):
    for i in PAIR:
        out[span(i, WIDE), span(s, n_tok)] = dot(pt_ref[0, i, s], values_ref[span(s, n_tok), span(i, LANES)], NT).astype(BF16)


def first_kernel(n_tok, u_ref, p_ref, pt_ref, *refs):
    g_refs, x_refs, dy_refs = (refs[span(i, N_SET)] for i in range(3))
    uc_ref, w_ref, s_ref, dv_ref, wrt, pre = refs[3 * N_SET:]
    tok_chunk = min(TOK_STEP, n_tok)

    def front(s):
        for part in halves(n_tok):
            pre[s, part, :] = dot(x_refs[s][part, :], uc_ref[0, s], NT)

    def back(s):
        for t in range(n_tok // tok_chunk):
            rows = span(s * (n_tok // tok_chunk) + t, tok_chunk)
            for i in PAIR:
                gate = g_refs[s][span(t, tok_chunk // TILE), i].reshape(tok_chunk, LANES)
                act, slope = gelu_pair(pre[s, span(t, tok_chunk), span(i, LANES)])
                used = gate > 0.0
                w_ref[rows, span(i, LANES)] = jnp.where(used, gate * act, 0.0).astype(BF16)
                s_ref[rows, span(i, LANES)] = jnp.where(used, gate * slope, 0.0)
        spread_slots(pt_ref, w_ref, wrt, s, n_tok)

    pick_rows(p_ref, [u_ref[span(i, WIDE), :] for i in PAIR], uc_ref)
    staggered(front, back)
    dy_all = jnp.concatenate([ref[...] for ref in dy_refs], axis=0)
    dv_ref[...] = dot(wrt[...], dy_all).astype(BF16)


def first_pass(u_all, p_hot, pt_hot, gates, xs, dys):
    n_tok, width = xs[0].shape
    all_tok, slots = N_SET * n_tok, N_GRP * WIDE
    flops = 2 * N_GRP * (N_SET * WIDE * WIDE * width + all_tok * (width * WIDE + LANES * G_ROWS + G_ROWS * width))
    return kernel(
        functools.partial(first_kernel, n_tok),
        arrays(BF16, (N_GRP, N_SET, WIDE, width), (all_tok, slots)) + arrays(F32, (all_tok, slots)) + arrays(BF16, u_all.shape),
        vmem(BF16, (G_ROWS, all_tok)) + vmem(F32, (N_SET, n_tok, WIDE)), flops, 76, grid=(N_GRP,),
        in_specs=[block((G_ROWS, width)), P_BLOCK, PT_BLOCK] + [block((n_tok // TILE, 2, TILE, LANES), axis=1)] * N_SET + [whole(one) for one in (*xs, *dys)],
        out_specs=[block((1, N_SET, WIDE, width)), block((all_tok, WIDE), axis=1), block((all_tok, WIDE), axis=1), block((G_ROWS, width))],
    )(u_all, p_hot, pt_hot, *gates, *xs, *dys)


def down_kernel(n_tok, v_ref, vf_ref, p_ref, w_ref, vc_ref, *y_refs):
    @pl.when(pl.program_id(0) == 0)
    def _():
        for y_ref in y_refs:
            y_ref[...] = jnp.zeros_like(y_ref)

    pick_rows(p_ref, [jnp.concatenate([ref[span(i, ROWS), :] for ref in (v_ref, vf_ref)], axis=0) for i in PAIR], vc_ref)
    for s in SETS:
        y_refs[s][...] += dot(w_ref[span(s, n_tok), :], vc_ref[0, s])


def down_pass(v_own, v_far, p_hot, w_all):
    width = v_own.shape[1]
    all_tok = w_all.shape[0]
    n_tok = all_tok // N_SET
    flops = 2 * N_GRP * WIDE * width * (N_SET * WIDE + all_tok)
    return kernel(
        functools.partial(down_kernel, n_tok),
        arrays(BF16, (N_GRP, N_SET, WIDE, width)) + arrays(F32, *[(n_tok, width)] * N_SET), [], flops, 44, grid=(N_GRP,),
        in_specs=[block((2 * ROWS, width))] * 2 + [P_BLOCK, block((all_tok, WIDE), axis=1)],
        out_specs=[block((1, N_SET, WIDE, width))] + [block((n_tok, width), axis=None)] * N_SET,
    )(v_own, v_far, p_hot, w_all)


def second_kernel(n_tok, vc_ref, pt_ref, s_ref, *refs):
    x_refs, dy_refs = (refs[span(i, N_SET)] for i in PAIR)
    c_ref, du_ref, crt = refs[2 * N_SET:]

    def front(s):
        for part in halves(n_tok):
            rows = slice(s * n_tok + part.start, s * n_tok + part.stop)
            back_dot = dot(dy_refs[s][part, :], vc_ref[0, s], NT)
            slope = s_ref[rows, :]
            c_ref[rows, :] = jnp.where(slope == 0.0, 0.0, slope * back_dot).astype(BF16)

    staggered(front, lambda s: spread_slots(pt_ref, c_ref, crt, s, n_tok))
    x_all = jnp.concatenate([ref[...] for ref in x_refs], axis=0)
    du_ref[...] = dot(crt[...], x_all).astype(BF16)


def second_pass(vc, pt_hot, slopes, xs, dys):
    n_tok, width = xs[0].shape
    all_tok = N_SET * n_tok
    flops = 2 * N_GRP * all_tok * (width * WIDE + LANES * G_ROWS + G_ROWS * width)
    return kernel(
        functools.partial(second_kernel, n_tok),
        arrays(BF16, slopes.shape, (N_GRP * G_ROWS, width)), vmem(BF16, (G_ROWS, all_tok)), flops, 58, grid=(N_GRP,),
        in_specs=[block((1, N_SET, WIDE, width)), PT_BLOCK, block((all_tok, WIDE), axis=1)] + [whole(one) for one in (*xs, *dys)],
        out_specs=[block((all_tok, WIDE), axis=1), block((G_ROWS, width))],
    )(vc, pt_hot, slopes, *xs, *dys)


HALVES = (OPP, NEXT), (PREV, OWN)
FAR_STEP, PLAIN, SUMMED, FAR_2, PLAIN_2, SUMMED_2, PLANE, N_MSG = 0, 4, 8, 12, 14, 16, 18, 19
N_TILE, CHUNK = 4, 32


def tail_kernel(part_ref, c_ref, uc_ref, out_ref, dx_ref,
                own_step, own_mid, s1, s2, sums, mid, t1, t2, tsum, keep, z_send, z_recv,
                c_buf, uc_buf, dx_part, core_recv, far_send, far_recv,
                send_sem, recv_sem, own_sem, load_sem, core_send_sem, core_recv_sem, far_send_sem, far_recv_sem):
    rows, width = out_ref.shape
    half = width // 2
    chip_rows = 2 * rows
    n_tok = dx_ref.shape[0]
    tile = n_tok // N_TILE
    at = Place()
    sides = at.sides

    def load_set(s):
        slot = s % 2
        return (pltpu.make_async_copy(c_ref.at[pl.ds(s * n_tok, n_tok)], c_buf.at[slot], load_sem.at[s, UP]),
                pltpu.make_async_copy(uc_ref.at[:, s], uc_buf.at[slot], load_sem.at[s, DOWN]))

    loads = [load_set(s) for s in SETS]
    for s in (SET_FAR_CORE, SET_FAR):
        start_all(loads[s])
    at.meet()

    def add_up(n_rows, store, *parts):
        def step(i):
            total = None
            for one_part in parts:
                term = one_part(i)
                total = term if total is None else total + term
            store(aligned(i * CHUNK, CHUNK), total)

        steps(n_rows // CHUNK, step)

    def from_buf(buf, *index, skip=0):
        return lambda i: buf[(*index, aligned(skip + i * CHUNK, CHUNK), slice(None))].astype(F32)

    def into_buf(buf, *index):
        def store(place, total):
            buf[(*index, place, slice(None))] = total.astype(buf.dtype)

        return store

    def own(one, shift1, shift2):
        return part_ref.at[aligned(chip_at(one, shift1, shift2) * chip_rows, chip_rows), pl.ds(one.k * half, half)]

    def message(one, number, src, dst, peer):
        return remote(src, dst, (send_sem, recv_sem), (one.k, number), peer)

    plane_rows = (pl.ds(0, rows), pl.ds(rows, rows))
    STEP = NEXT, PREV
    for one in sides:
        k = one.k
        one.far1 = [[message(one, FAR_STEP + d * 2 + i, own(one, OPP, r), s1.at[k, d, i], one.axis1[d]) for i, r in enumerate(HALVES[d])] for d in PAIR]
        one.plain1 = [[message(one, PLAIN + d * 2 + i, own(one, STEP[d], r), s2.at[k, d, r], one.axis1[d]) for i, r in enumerate(HALVES[1 - d])] for d in PAIR]
        one.summed1 = [[message(one, SUMMED + d * 2 + i, sums.at[k, d, i], s2.at[k, d, r], one.axis1[d]) for i, r in enumerate(HALVES[d])] for d in PAIR]
        one.far2 = [message(one, FAR_2 + d, mid.at[k, OPP, plane_rows[d]], t1.at[k, d], one.axis2[d]) for d in PAIR]
        one.plain2 = [message(one, PLAIN_2 + d, mid.at[k, STEP[d], plane_rows[1 - d]], t2.at[k, d, 1 - d], one.axis2[d]) for d in PAIR]
        one.summed2 = [message(one, SUMMED_2 + d, tsum.at[k, d], t2.at[k, d, d], one.axis2[d]) for d in PAIR]
        one.plane = message(one, PLANE, z_send.at[k], z_recv.at[k], at.plane_peer)
        one.stage = [pltpu.make_async_copy(own(one, STEP[d], r), own_step.at[k, d, i], own_sem.at[k, d * 2 + i]) for d in PAIR for i, r in enumerate(HALVES[d])]
        one.stage += [pltpu.make_async_copy(own(one, OWN, r), own_mid.at[k, r], own_sem.at[k, RING + r]) for r in range(RING)]

    def tile_at(t):
        return aligned(t * tile, tile)

    def core_msg(which, t):
        return remote(dx_part.at[SET_CORE if which else SET_FAR_CORE, tile_at(t)], core_recv.at[which, tile_at(t)],
                      (core_send_sem, core_recv_sem), (which, t), at.core_peer)

    def far_msg(t):
        return remote(far_send.at[tile_at(t)], far_recv.at[tile_at(t)], (far_send_sem, far_recv_sem), t, at.far_peer)

    def dx_tile(s, t):
        dx_part[s, tile_at(t), :] = dot(c_buf[s % 2, tile_at(t), :], uc_buf[s % 2].reshape(N_GRP * WIDE, width))

    def dx_pair(which, sets):
        for s in sets:
            wait_all(loads[s])

        def step(t):
            dx_tile(sets[UP], t)
            core_msg(which, t).start()
            dx_tile(sets[DOWN], t)

        steps(N_TILE, step)

    def row_steps(t, body):
        steps(tile // CHUNK, lambda i: body(aligned(t * tile + i * CHUNK, CHUNK)))

    for kind in ('far1', 'plain1'):
        for i in PAIR:
            for one in sides:
                for d in PAIR:
                    getattr(one, kind)[d][i].start()
    for one in sides:
        start_all(one.stage)

    dx_pair(UP, (SET_FAR_CORE, SET_FAR))
    for s in (SET_CORE, SET_ME):
        start_all(loads[s])

    def far_sum(t):
        core_msg(UP, t).wait_recv()

        def add(place):
            far_send[place, :] = dx_part[SET_FAR, place, :] + core_recv[UP, place, :]

        row_steps(t, add)
        far_msg(t).start()

    steps(N_TILE, far_sum)

    for one in sides:
        wait_all(one.stage)
    for i in PAIR:
        for one in sides:
            for d in PAIR:
                one.far1[d][i].wait_recv()
                add_up(chip_rows, into_buf(sums, one.k, d, i), from_buf(own_step, one.k, d, i), from_buf(s1, one.k, d, i))
                one.summed1[d][i].start()

    dx_pair(DOWN, (SET_CORE, SET_ME))

    for i in PAIR:
        for half_way in PAIR:
            r = HALVES[half_way][i]
            for one in sides:
                k = one.k
                one.plain1[1 - half_way][i].wait_recv()
                one.summed1[half_way][i].wait_recv()
                add_up(chip_rows, into_buf(mid, k, r), from_buf(own_mid, k, r), from_buf(s2, k, UP, r), from_buf(s2, k, DOWN, r))
                if r == OPP:
                    start_all(one.far2)
                elif r != OWN:
                    one.plain2[STEP.index(r)].start()
    for one in sides:
        k = one.k
        for d in PAIR:
            one.far2[d].wait_recv()
            add_up(rows, into_buf(tsum, k, d), from_buf(mid, k, STEP[d], skip=d * rows), from_buf(t1, k, d))
            one.summed2[d].start()
    for one in sides:
        k = one.k
        for msg in one.plain2 + one.summed2:
            msg.wait_recv()
        add_up(rows, into_buf(z_send, k), from_buf(mid, k, OWN, skip=rows), from_buf(t2, k, UP, THERE), from_buf(t2, k, DOWN, THERE))
        one.plane.start()
        add_up(rows, into_buf(keep, k), from_buf(mid, k, OWN), from_buf(t2, k, UP, HERE), from_buf(t2, k, DOWN, HERE))
    for one in sides:
        k = one.k
        one.plane.wait_recv()

        def store_out(place, total, k=k):
            out_ref[place, span(k, half)] = total.astype(BF16)

        add_up(rows, store_out, from_buf(keep, k), from_buf(z_recv, k))

    def last_tile(t):
        core_msg(DOWN, t).wait_recv()
        far_msg(t).wait_recv()

        def add(place):
            dx_ref[place, :] = (dx_part[SET_ME, place, :] + core_recv[DOWN, place, :] + far_recv[place, :]).astype(BF16)

        row_steps(t, add)

    steps(N_TILE, last_tile)

    def sent(t):
        for which in PAIR:
            core_msg(which, t).wait_send()
        far_msg(t).wait_send()

    steps(N_TILE, sent)
    for one in sides:
        for pairs in (one.far1, one.plain1, one.summed1):
            for msg in pairs[UP] + pairs[DOWN]:
                msg.wait_send()
        for msg in one.far2 + one.plain2 + one.summed2 + [one.plane]:
            msg.wait_send()


def tail_pass(part, c_all, uc):
    width = part.shape[1]
    rows = part.shape[0] // N_OWN
    n_tok = c_all.shape[0] // N_SET
    half = width // 2
    big, small, toks = (2 * rows, half), (rows, half), (n_tok, width)
    scratch = vmem(BF16, (2, 2, 2, *big), (2, RING, *big), (2, 2, 2, *big), (2, 2, RING, *big), (2, 2, 2, *big), (2, RING, *big), (2, 2, *small), (2, 2, 2, *small), (2, 2, *small))
    scratch += vmem(F32, (2, *small)) + vmem(BF16, (2, *small), (2, *small), (2, n_tok, N_GRP * WIDE), (2, N_GRP, WIDE, width))
    scratch += vmem(F32, (N_SET, *toks), (2, *toks), toks, toks)
    messages, tiles = (2, N_MSG), (2, N_TILE)
    scratch += dma_sems(messages, messages, (2, 2 * RING), (N_SET, 2), tiles, tiles, (N_TILE,), (N_TILE,))
    return kernel(
        tail_kernel, arrays(BF16, (rows, width), toks), scratch, 2 * c_all.size * width, 40, comm=0,
        in_specs=[ANY] * 3, out_specs=[IN_VMEM] * 2)(part, c_all, uc)


def solution(mesh):
    tok_spec, table_spec = P(('dp', 'ep')), P('ep')
    plane = [[z * N_OWN + yx * 2 + c for yx in range(CHIPS)] for z in range(RING) for c in PAIR]

    def swap(arr, mask):
        return lax.ppermute(arr, 'ep', [(i, i ^ mask) for i in range(N_EP)])

    def plane_rows(local):
        return lax.all_gather(local, 'ep', axis=0, tiled=True, axis_index_groups=plane)

    def device_part(tokens, slot_ids, request_rows, gate_vals, grad_out, up_local, down_local):
        n_tok = tokens.shape[0]
        meta = jnp.concatenate([slot_ids.reshape(n_tok, LANES).astype(F32), gate_vals.reshape(n_tok, LANES), request_rows.reshape(REQ, N_EP).astype(F32)])
        v_own = plane_rows(down_local)
        u_all, v_peer, xs, dys, gates, p_hot, pt_hot = head_pass(tokens, grad_out, meta, up_local, down_local)
        v_far = plane_rows(v_peer)
        uc, w_all, slopes, dv_part = first_pass(u_all, p_hot, pt_hot, gates, xs, dys)
        vc, y_own, y_core, y_far, y_far_core = down_pass(v_own, v_far, p_hot, w_all)
        y_for_far, vc = lax.optimization_barrier((y_far + swap(y_far_core, CORE), vc))
        y_from_far = swap(y_for_far, ZTOK)
        y_from_core = swap(y_core, CORE)
        c_all, du_part = second_pass(vc, pt_hot, slopes, xs, dys)
        grad_up, dx = tail_pass(du_part, c_all, uc)
        dv_mine = lax.psum_scatter(dv_part, 'ep', scatter_dimension=0, tiled=True, axis_index_groups=plane)
        dv_mine, y_own, _ = lax.optimization_barrier((dv_mine, y_own, grad_up))
        dv_far = swap(dv_mine[ROWS:], ZTAB)
        y = (y_own + y_from_core + y_from_far).astype(BF16)
        grad_down = (dv_mine[:ROWS].astype(F32) + dv_far.astype(F32)).astype(BF16)
        return y, dx, grad_up, grad_down

    return jax.shard_map(device_part, mesh=mesh, in_specs=(tok_spec,) * 5 + (table_spec,) * 2, out_specs=(tok_spec,) * 4, check_vma=False)
```
